32 devices in a mesh: row: 4 (over y, core), col: 8 (over z, x).
Axes of the slice: x: 2, y: 2, z: 4, core: 2. Of those that a mesh axis runs over, the one named last changes fastest.
Arguments:
- parent_front: float32 [8, 1024, 4, 2048], P(None, 'row', None, 'col'), may hold values from -6 to 6
- generators: bfloat16 [48, 256, 256], P('row'), may hold values from -1.5 to 1.5
- diagonal_blocks: bfloat16 [48, 256, 256], P('row'), may hold values from -6 to 6
- coupling: bfloat16 [2, 256, 256], replicated, may hold values from -0.375 to 0.375
- block_map: int32 [2, 24], replicated, may hold values from 0 to 31, as said below
- valid_rows: int32 [2, 24], replicated, may hold values from 128 to 256
Outputs:
- assembled: float32 [8, 1024, 4, 2048], P(None, 'row', None, 'col')
The draws below stay inside these ranges and needn't reach their ends.
Inputs may be any that keep to these rules, and one draw needn't show every extreme that they name: `block_map`: for each child c and each s < 2, the child blocks s * 12 to (s + 1) * 12 - 1 map in increasing order to distinct parent blocks of the range s * 16 to (s + 1) * 16 - 1, and the parent blocks s * 16 + m * 4 of that range always receive one.
All inputs are finite; a program needn't handle non-finite values.
Results may differ from the reference program's by a relative error of at most 0.0028.
Values may be sent and summed in bfloat16 or wider, within the bound.
A program may use at most 128 MiB of HBM per device.

```python
import jax
import jax.numpy as jnp
from jax import lax

BLK = 256
RANK = 256
BR_DEV = 8
PB = 32
BC_DEV = 4
WIN = 16
CG = 12
HALF = 2
CB = 24
N_ROW = 4
N_COL = 8


def draw_block_map(key, part):
    child_rows = []
    for child_index in range(2):
        pieces = []
        for group_index in range(HALF):
            window_key = jax.random.fold_in(key, 1000 * child_index + group_index + 17)
            offsets = jnp.arange(WIN, dtype=jnp.int32)
            scores = jax.random.randint(window_key, (WIN,), 0, 1 << 20, dtype=jnp.int32) * WIN + offsets
            scores = jnp.where(offsets % N_ROW == 0, jnp.int32(1 << 30), scores)
            gap_order = jnp.argsort(scores, stable=True)
            gap_slots = gap_order[:WIN - CG]
            gap_flags = jnp.zeros((WIN,), jnp.int32).at[gap_slots].set(1)
            sorted_slots = jnp.argsort(gap_flags * WIN + offsets, stable=True).astype(jnp.int32)
            chosen = sorted_slots[:CG] + WIN * group_index
            pieces.append(chosen)
        child_rows.append(jnp.concatenate(pieces))
    return jnp.stack(child_rows).astype(jnp.int32)


def place_ends(entries, own_key, low, high):
    longest = entries.shape.index(max(entries.shape))
    spots = []
    for shift in (0, 1):
        where = [jax.random.randint(jax.random.fold_in(own_key, axis), (), 0, length) for axis, length in enumerate(entries.shape)]
        where[longest] = (where[longest] + shift) % entries.shape[longest]
        spots.append(tuple(where))
    return entries.at[spots[0]].set(low).at[spots[1]].set(high)


def shard_levels(own_key, extent, cuts, smallest, largest):
    def one(dim, blocks):
        heights = jax.random.uniform(jax.random.fold_in(jax.random.fold_in(own_key, 6), dim), (blocks,), jnp.float32, smallest / len(cuts), largest / len(cuts))
        return jnp.repeat(jnp.exp(heights), extent[dim] // blocks).reshape((-1,) + (1,) * (len(extent) - dim - 1))

    loudness = one(*cuts[0])
    for cut in cuts[1:]:
        loudness = loudness * one(*cut)
    return loudness


def bell_draw(stream_key, dims, scale, reach, cuts=(), held_as=jnp.bfloat16):
    entries = jax.random.normal(stream_key, dims, jnp.float32) * scale
    if len(cuts) > 0:
        entries = shard_levels(stream_key, dims, cuts, -0.22, 0.18) * entries
    return jnp.clip(entries, min=-reach, max=reach).astype(held_as)


def setup_inputs(seed: int = 0) -> dict:
    arg_keys = jax.random.split(jax.random.key(seed), 7)
    parent_front = bell_draw(arg_keys[0], (BR_DEV, N_ROW * BLK, BC_DEV, N_COL * BLK), 1.0, 6.0, ((1, 4), (3, 8)), jnp.float32)
    generators = bell_draw(arg_keys[1], (2 * CB, BLK, RANK), 0.25, 1.5, ((0, 4),))
    diagonal_blocks = bell_draw(arg_keys[2], (2 * CB, BLK, BLK), 1.0, 6.0, ((0, 4),))
    coupling = bell_draw(arg_keys[3], (2, RANK, RANK), RANK ** -0.5, 0.375)
    block_map = draw_block_map(jax.random.fold_in(arg_keys[6], 71), 0)
    valid_rows = place_ends(jax.random.randint(arg_keys[5], (2, CB), BLK // 2, BLK + 1), jax.random.fold_in(arg_keys[5], 1), BLK // 2, BLK).astype(jnp.int32)
    return dict(parent_front=parent_front, generators=generators, diagonal_blocks=diagonal_blocks, coupling=coupling, block_map=block_map, valid_rows=valid_rows)


def child_select(stacked, child_index):
    grouped = stacked.reshape((HALF, 2, CG) + stacked.shape[1:])
    return grouped[:, child_index].reshape((CB,) + stacked.shape[1:])


def child_parts(gen_blocks, diag_rows, coupling_one, map_row, count_row):
    row_offsets = jnp.arange(BLK, dtype=jnp.int32)
    kept_mask = (row_offsets[None, :] < count_row[:, None]).astype(jnp.float32)
    masked = gen_blocks.astype(jnp.float32) * kept_mask[:, :, None]
    projected = jnp.einsum("ixq,qr->ixr", masked, coupling_one.astype(jnp.float32)).astype(jnp.bfloat16)
    diag_kept = diag_rows.astype(jnp.float32) * kept_mask[:, :, None] * kept_mask[:, None, :]
    placing = (map_row[None, :] == jnp.arange(PB, dtype=jnp.int32)[:, None]).astype(jnp.float32)
    placed_gen = jnp.einsum("pi,ixq->pxq", placing, masked)
    placed_proj = jnp.einsum("pi,ixq->pxq", placing, projected.astype(jnp.float32))
    placed_diag = jnp.einsum("pi,ixz->pxz", placing, diag_kept)
    return placed_gen, placed_proj, placed_diag


def reference(parent_front, generators, diagonal_blocks, coupling, block_map, valid_rows):
    front_blocks = parent_front.reshape(PB, BLK, PB, BLK)
    child_data = [child_parts(child_select(generators, child_index),
                              child_select(diagonal_blocks, child_index),
                              coupling[child_index], block_map[child_index], valid_rows[child_index])
                  for child_index in range(2)]
    placed_gen = jnp.stack([child_data[0][0], child_data[1][0]], axis=1)
    placed_proj = jnp.stack([child_data[0][1], child_data[1][1]])
    placed_diag = jnp.stack([child_data[0][2], child_data[1][2]], axis=1)
    block_ids = jnp.arange(PB, dtype=jnp.int32)

    def one_row(row_items):
        front_row, gen_row, diag_row, row_id = row_items
        on_diag = (block_ids == row_id).astype(jnp.float32)
        running = front_row
        for child_index in range(2):
            child_tile = jnp.einsum("xq,jzq->xjz", gen_row[child_index], placed_proj[child_index])
            child_tile = child_tile + diag_row[child_index][:, None, :] * on_diag[None, :, None]
            rounded = lax.optimization_barrier(child_tile.astype(jnp.bfloat16))
            running = running + rounded.astype(jnp.float32)
        return running

    rows_out = lax.map(one_row, (front_blocks, placed_gen, placed_diag, block_ids))
    return rows_out.reshape(BR_DEV, N_ROW * BLK, BC_DEV, N_COL * BLK)
```

```python
import functools

import jax
import jax.numpy as jnp
from jax import lax
from jax.experimental import pallas as pl
from jax.experimental.pallas import tpu as pltpu
from jax.sharding import PartitionSpec as P

MESH = pl.DeviceIdType.MESH
QUAD = 4
LANES = 128
PIECES = 2
LAG = 2


def exchange_kernel(
    row_count, col_count, row_cap, col_cap,
    gen_hbm, diag_hbm, coupling_hbm, map_hbm, count_hbm, front_hbm,
    rows_out, cols_out, diag_out, front_out,
    gen_ref, diag_ref, coupling_ref, map_ref, count_ref, load_sem, front_sem,
    far_rows, pair_rows, own_diag,
    far_send, far_recv, x_send, x_recv, z_send, z_recv, xr_send, xr_recv, zr_send, zr_recv,
    pair_send, pair_recv, near_send, near_recv, col_send, col_recv, fwd_send, fwd_recv,
    over_send, over_recv, diag_send, diag_recv,
):
    groups = row_count // 2
    group_blocks, block, rank = gen_ref.shape
    window = row_cap * row_count
    rows_of = block // PIECES
    steps = [(t, p) for t in range(col_cap) for p in range(PIECES)]
    row = lax.axis_index("row")
    col = lax.axis_index("col")
    group = row // 2
    core = row % 2
    quarter = col % QUAD
    half = col // row_count
    pair_row = group * 2 + 1 - core
    diag_row = col % row_count
    x_col = col + 1 - 2 * (quarter % 2)
    z_col = col + 2 - 4 * (quarter // 2)
    holder = quarter % 2 == core

    def parity(dest):
        return jnp.where(quarter // 2 == dest % 2, half, 1 - half)

    def overlaps(dest):
        return diag_row // 2 == dest

    def lookup(child, source, slot):
        found = jnp.int32(0)
        count = jnp.int32(0)
        target = source * window + slot
        for d in range(window - group_blocks + 1):
            k = jnp.clip(slot - d, 0, group_blocks - 1)
            hit = map_ref[child, source * group_blocks + k] == target
            found = jnp.where(hit, k, found)
            count = jnp.where(hit, count_ref[child, source * group_blocks + k], count)
        return found, count

    row_iota = lax.broadcasted_iota(jnp.int32, (block, LANES), 0)

    def masked_rows(slot):
        found, count = lookup(core, group, slot)
        kept = (row_iota < count).astype(jnp.float32).astype(jnp.bfloat16)
        return gen_ref[found] * jnp.concatenate([kept] * (rank // LANES), axis=1)

    def project(child, rows):
        return lax.dot_general(
            coupling_ref[child], rows, (((0,), (1,)), ((), ())),
            preferred_element_type=jnp.float32,
        ).astype(jnp.bfloat16)

    def remote(src, dst, send, recv, to_row, to_col):
        return pltpu.make_async_remote_copy(
            src_ref=src, dst_ref=dst, send_sem=send, recv_sem=recv,
            device_id=(to_row, to_col), device_id_type=MESH,
        )

    def load(src, dst, n):
        return pltpu.make_async_copy(src, dst, load_sem.at[n])

    loads = [
        load(src, dst, n)
        for n, (src, dst) in enumerate((
            (map_hbm, map_ref), (count_hbm, count_ref), (gen_hbm, gen_ref),
            (coupling_hbm, coupling_ref), (diag_hbm, diag_ref),
        ))
    ]
    for copy in loads:
        copy.start()

    barrier = pltpu.get_barrier_semaphore()
    for k in range(1, row_count):
        pl.semaphore_signal(
            barrier, inc=1, device_id=((row + k) % row_count, col), device_id_type=MESH
        )
    for other in (x_col, z_col):
        pl.semaphore_signal(barrier, inc=1, device_id=(row, other), device_id_type=MESH)

    def far_copy(k, child, source, par, t, p, dest_row):
        part = pl.ds(p * rows_of, rows_of)
        return remote(
            far_rows.at[k - 1, t, part], rows_out.at[source, 2 * t + par, child, part],
            far_send.at[k - 1, t, p], far_recv.at[k - 1, child, t, p], dest_row, col,
        )

    def landed(source, par, child, t, p):
        return rows_out.at[source, 2 * t + par, child, pl.ds(p * rows_of, rows_of)]

    def x_copy(k, source, par, child, t, p):
        piece = landed(source, par, child, t, p)
        at = (k - 1, child, t, p)
        return remote(piece, piece, x_send.at[at], x_recv.at[at], row, x_col)

    def z_copy(k, source, par, child, t, p):
        piece = landed(source, par, child, t, p)
        at = (k - 1, child, t, p)
        return remote(piece, piece, z_send.at[at], z_recv.at[at], row, z_col)

    def xr_copy(k, source, par, t, p):
        piece = landed(source, par, 0, t, p)
        at = (k - 1, t, p)
        return remote(piece, piece, xr_send.at[at], xr_recv.at[at], row, x_col)

    def zr_copy(k, source, par, t, p):
        piece = landed(source, par, 1, t, p)
        at = (k - 1, t, p)
        return remote(piece, piece, zr_send.at[at], zr_recv.at[at], row, z_col)

    def pair_copy(child, m):
        return remote(
            pair_rows.at[m], rows_out.at[group, m, child],
            pair_send.at[m], pair_recv.at[m], pair_row, col,
        )

    def near_copy(child, t):
        piece = cols_out.at[group, t, child]
        return remote(piece, piece, near_send.at[t], near_recv.at[t], pair_row, col)

    def col_copy(k, source, t, dest):
        piece = cols_out.at[source, t, core]
        return remote(
            piece, piece, col_send.at[k - 1, t], col_recv.at[k - 1, t], 2 * dest + core, col
        )

    def fwd_copy(k, source, child, t):
        piece = cols_out.at[source, t, child]
        return remote(piece, piece, fwd_send.at[k - 1, t], fwd_recv.at[k - 1, t], pair_row, col)

    def over_copy(k, source, child, t):
        piece = cols_out.at[source, t, child]
        at = (k - 1, child, t)
        return remote(piece, piece, over_send.at[at], over_recv.at[at], pair_row, col)

    def diag_copy(source, child, t):
        return remote(
            own_diag.at[t], diag_out.at[source, child, t],
            diag_send.at[t], diag_recv.at[source, child, t], diag_row, col,
        )

    far = [(k, (group + k) % groups) for k in range(1, groups)]
    sources = [(k, (group + groups - k) % groups) for k in range(1, groups)]
    par = parity(group)

    for copy in loads[:3]:
        copy.wait()
    for t in range(col_cap):
        for k, dest in far:
            slot = (2 * t + parity(dest)) * row_count + 2 * dest + quarter % 2
            far_rows[k - 1, t] = masked_rows(slot)
        if t == 0:
            pl.semaphore_wait(barrier, row_count + 1)
        for k, dest in far:
            for p in range(PIECES):
                far_copy(k, core, group, parity(dest), t, p, 2 * dest + quarter % 2).start()

    front_loads = [
        pltpu.make_async_copy(front_hbm.at[a, :, h], front_out.at[a, h], front_sem.at[a, h])
        for a in range(front_out.shape[0]) for h in range(front_out.shape[1])
    ]
    for copy in loads[3:]:
        copy.wait()

    for t in range(col_cap):
        cols_out[group, t, core] = project(core, masked_rows(t * col_count + col))
        near_copy(core, t).start()
        for k, dest in far:
            @pl.when(jnp.logical_not(overlaps(dest)))
            def _():
                col_copy(k, group, t, dest).start()

    row_iota2 = lax.broadcasted_iota(jnp.int32, (block, block), 0)
    col_iota2 = lax.broadcasted_iota(jnp.int32, (block, block), 1)
    edge = jnp.maximum(row_iota2, col_iota2)
    for t in range(col_cap):
        found, count = lookup(core, group, t * col_count + col)
        piece = jnp.where(edge < count, diag_ref[found].astype(jnp.float32), 0.0)
        own_diag[t] = piece.astype(jnp.bfloat16)

        @pl.when(row != diag_row)
        def _():
            diag_copy(group, core, t).start()

        @pl.when(row == diag_row)
        def _():
            diag_out[group, core, t] = own_diag[t]

    for copy in front_loads:
        copy.start()
    for m in range(row_cap):
        pair_rows[m] = masked_rows(m * row_count + pair_row)
        pair_copy(core, m).start()
    for m in range(row_cap):
        rows_out[group, m, core] = masked_rows(m * row_count + row)

    @pl.when(holder)
    def _():
        for i in range(len(steps) + LAG):
            if i < len(steps):
                t, p = steps[i]
                for k, source in sources:
                    for child in range(2):
                        far_copy(k, child, source, par, t, p, row).wait_recv()
                        x_copy(k, source, par, child, t, p).start()
                        z_copy(k, source, par, child, t, p).start()
            if i >= LAG:
                t, p = steps[i - LAG]
                for k, source in sources:
                    z_copy(k, source, 1 - par, 0, t, p).wait_recv()
                    xr_copy(k, source, 1 - par, t, p).start()
            if i == len(steps) - 1:
                @pl.when(overlaps(group))
                def _():
                    for k, source in sources:
                        for t in range(col_cap):
                            for child in range(2):
                                cols_out[source, t, child] = project(
                                    child, rows_out[source, 2 * t + par, child]
                                )
                                over_copy(k, source, child, t).start()

    @pl.when(jnp.logical_not(holder))
    def _():
        for t, p in steps:
            for k, source in sources:
                x_copy(k, source, par, 1, t, p).wait_recv()
                zr_copy(k, source, par, t, p).start()
                x_copy(k, source, par, 0, t, p).wait_recv()

    @pl.when(jnp.logical_not(overlaps(group)))
    def _():
        for t in range(col_cap):
            for k, source in sources:
                col_copy(k, source, t, group).wait_recv()
                fwd_copy(k, source, core, t).start()

    for copy in front_loads:
        copy.wait()
    for m in range(row_cap):
        pair_copy(1 - core, m).wait_recv()
        pair_copy(core, m).wait_send()
    for t in range(col_cap):
        near_copy(1 - core, t).wait_recv()
        near_copy(core, t).wait_send()
    for k, dest in far:
        for t, p in steps:
            far_copy(k, core, group, 0, t, p, row).wait_send()

    @pl.when(row == diag_row)
    def _():
        for source in range(groups):
            for child in range(2):
                @pl.when(2 * source + child != row)
                def _():
                    for t in range(col_cap):
                        diag_copy(source, child, t).wait_recv()

    @pl.when(row != diag_row)
    def _():
        for t in range(col_cap):
            diag_copy(group, core, t).wait_send()

    for k, dest in far:
        @pl.when(jnp.logical_not(overlaps(dest)))
        def _():
            for t in range(col_cap):
                col_copy(k, group, t, dest).wait_send()

    @pl.when(holder)
    def _():
        for t, p in steps:
            for k, source in sources:
                z_copy(k, source, 1 - par, 1, t, p).wait_recv()
                xr_copy(k, source, 1 - par, t, p).wait_send()
                for child in range(2):
                    x_copy(k, source, par, child, t, p).wait_send()
                    z_copy(k, source, par, child, t, p).wait_send()

    @pl.when(jnp.logical_not(holder))
    def _():
        for t, p in steps:
            for k, source in sources:
                zr_copy(k, source, par, t, p).wait_send()
                zr_copy(k, source, 1 - par, t, p).wait_recv()
                xr_copy(k, source, 1 - par, t, p).wait_recv()

    @pl.when(overlaps(group))
    def _():
        @pl.when(holder)
        def _():
            for k, source in sources:
                for t in range(col_cap):
                    for child in range(2):
                        over_copy(k, source, child, t).wait_send()

        @pl.when(jnp.logical_not(holder))
        def _():
            for k, source in sources:
                for t in range(col_cap):
                    for child in range(2):
                        over_copy(k, source, child, t).wait_recv()

    @pl.when(jnp.logical_not(overlaps(group)))
    def _():
        for t in range(col_cap):
            for k, source in sources:
                fwd_copy(k, source, 1 - core, t).wait_recv()
                fwd_copy(k, source, core, t).wait_send()


def add_kernel(
    row_count, col_count, front_ref, rows_ref, cols_ref, diag_ref, out_ref, staged, out_sem
):
    rows_local, halves, block, cols_local, _ = front_ref.shape
    _, row_cap, _, _, rank = rows_ref.shape
    col_cap = cols_ref.shape[1]
    ratio = col_count // row_count
    row = lax.axis_index("row")
    col = lax.axis_index("col")

    def write(a, h):
        return pltpu.make_async_copy(staged.at[a, h], out_ref.at[a, :, h], out_sem.at[a, h])

    for a in range(rows_local):
        s, m = divmod(a, row_cap)
        rows = jnp.concatenate([rows_ref[s, m, 0], rows_ref[s, m, 1]], axis=1)
        for b in range(cols_local):
            cols = cols_ref[b // col_cap, b % col_cap].reshape(2 * rank, block)
            tile = jnp.dot(rows, cols, preferred_element_type=jnp.float32)
            spot = pl.ds(b, block, stride=cols_local)
            for h in range(halves):
                src = front_ref.at[a, h].reshape(block * cols_local, LANES)
                dst = staged.at[a, h].reshape(block * cols_local, LANES)
                dst[spot, :] = src[spot, :] + tile[:, h * LANES:(h + 1) * LANES]

        @pl.when((a % ratio) * row_count + row == col)
        def _():
            b = a // ratio
            s, t = divmod(b, col_cap)
            piece = diag_ref[s, 0, t].astype(jnp.float32) + diag_ref[s, 1, t].astype(jnp.float32)
            spot = pl.ds(b, block, stride=cols_local)
            for h in range(halves):
                dst = staged.at[a, h].reshape(block * cols_local, LANES)
                dst[spot, :] = dst[spot, :] + piece[:, h * LANES:(h + 1) * LANES]

        for h in range(halves):
            write(a, h).start()
    for a in range(rows_local):
        for h in range(halves):
            write(a, h).wait()


def shards(parent_front, generators, diagonal_blocks, coupling, block_map, valid_rows):
    row_count = lax.axis_size("row")
    col_count = lax.axis_size("col")
    groups = row_count // 2
    block, rank = generators.shape[1:]
    rows_local = parent_front.shape[0]
    cols_local = parent_front.shape[2]
    row_cap = rows_local // groups
    col_cap = cols_local // groups
    vmem = pl.BlockSpec(memory_space=pltpu.VMEM)
    hbm = pl.BlockSpec(memory_space=pltpu.HBM)
    dma = pltpu.SemaphoreType.DMA
    halves = block // LANES
    split = parent_front.reshape(rows_local, block, cols_local, halves, LANES)
    split = split.transpose(0, 1, 3, 2, 4)
    held = (rows_local, halves, block, cols_local, LANES)
    operands = [
        pltpu.with_memory_space_constraint(x, pltpu.HBM)
        for x in (generators, diagonal_blocks, coupling, block_map, valid_rows, split)
    ]
    far = groups - 1
    pieces = (far, 2, col_cap, PIECES)
    relays = (far, col_cap, PIECES)
    rows, cols, diag, front = pl.pallas_call(
        functools.partial(exchange_kernel, row_count, col_count, row_cap, col_cap),
        out_shape=(
            pltpu.VMEM((groups, row_cap, 2, block, rank), jnp.bfloat16),
            pltpu.VMEM((groups, col_cap, 2, rank, block), jnp.bfloat16),
            pltpu.VMEM((groups, 2, col_cap, block, block), jnp.bfloat16),
            pltpu.VMEM(held, jnp.float32),
        ),
        in_specs=[hbm] * 6,
        out_specs=(vmem,) * 4,
        scratch_shapes=[
            pltpu.VMEM(generators.shape, jnp.bfloat16),
            pltpu.VMEM(diagonal_blocks.shape, jnp.bfloat16),
            pltpu.VMEM(coupling.shape, jnp.bfloat16),
            pltpu.SMEM(block_map.shape, jnp.int32),
            pltpu.SMEM(valid_rows.shape, jnp.int32),
            dma((5,)),
            dma((rows_local, halves)),
            pltpu.VMEM((far, col_cap, block, rank), jnp.bfloat16),
            pltpu.VMEM((row_cap, block, rank), jnp.bfloat16),
            pltpu.VMEM((col_cap, block, block), jnp.bfloat16),
            dma(relays),
            dma(pieces),
            dma(pieces),
            dma(pieces),
            dma(pieces),
            dma(pieces),
            dma(relays),
            dma(relays),
            dma(relays),
            dma(relays),
            dma((row_cap,)),
            dma((row_cap,)),
            dma((col_cap,)),
            dma((col_cap,)),
            dma((far, col_cap)),
            dma((far, col_cap)),
            dma((far, col_cap)),
            dma((far, col_cap)),
            dma((far, 2, col_cap)),
            dma((far, 2, col_cap)),
            dma((col_cap,)),
            dma((groups, 2, col_cap)),
        ],
        compiler_params=pltpu.CompilerParams(
            collective_id=0, has_side_effects=True, vmem_limit_bytes=32 * 1024 * 1024
        ),
    )(*operands)
    out = pl.pallas_call(
        functools.partial(add_kernel, row_count, col_count),
        out_shape=jax.ShapeDtypeStruct(split.shape, jnp.float32),
        in_specs=[vmem] * 4,
        out_specs=hbm,
        scratch_shapes=[pltpu.VMEM(held, jnp.float32), dma((rows_local, halves))],
        compiler_params=pltpu.CompilerParams(vmem_limit_bytes=32 * 1024 * 1024),
    )(*(pltpu.with_memory_space_constraint(x, pltpu.VMEM) for x in (front, rows, cols, diag)))
    return out.transpose(0, 1, 3, 2, 4).reshape(parent_front.shape)


def solution(mesh):
    in_specs = (
        P(None, "row", None, "col"),
        P("row", None, None),
        P("row", None, None),
        P(),
        P(),
        P(),
    )
    out_specs = P(None, "row", None, "col")
    return jax.shard_map(shards, mesh=mesh, in_specs=in_specs, out_specs=out_specs, check_vma=False)
```

```python
import functools

import jax
import jax.numpy as jnp
from jax import lax
from jax.experimental import pallas as pl
from jax.experimental.pallas import tpu as pltpu
from jax.sharding import PartitionSpec as P

MESH = pl.DeviceIdType.MESH
QUAD = 4
LANES = 128


def steps_of(col_cap, block):
    unit = block // QUAD
    steps = []
    for t in range(col_cap):
        shape = (2, 2)
        if col_cap == 1:
            shape = (1, 1, 1, 1)
        elif t == 0:
            shape = (1, 1, 2)
        elif t == col_cap - 1:
            shape = (2, 1, 1)
        start = 0
        for size in shape:
            steps.append((t, start * unit, size * unit))
            start += size
    return steps


def exchange_kernel(
    row_count, col_count, row_cap, col_cap,
    gen_hbm, diag_hbm, coupling_hbm, map_hbm, count_hbm, front_hbm,
    rows_out, cols_out, front_out,
    gen_ref, diag_ref, coupling_ref, map_ref, count_ref, load_sem, front_sem,
    far_rows, pair_rows, own_diag, diag_in,
    far_send, far_recv, x_send, x_recv, z_send, z_recv, xr_send, xr_recv, zr_send, zr_recv,
    pair_send, pair_recv, near_send, near_recv, col_send, col_recv, fwd_send, fwd_recv,
    over_send, over_recv, diag_send, diag_recv,
):
    groups = row_count // 2
    group_blocks, block, rank = gen_ref.shape
    window = row_cap * row_count
    steps = steps_of(col_cap, block)
    middle = len(steps) // 2
    ratio = col_count // row_count
    cols_local = groups * col_cap
    row = lax.axis_index("row")
    col = lax.axis_index("col")
    group = row // 2
    core = row % 2
    quarter = col % QUAD
    half = col // row_count
    pair_row = group * 2 + 1 - core
    diag_row = col % row_count
    x_col = col + 1 - 2 * (quarter % 2)
    z_col = col + 2 - 4 * (quarter // 2)
    holder = quarter % 2 == core

    def parity(dest):
        return jnp.where(quarter // 2 == dest % 2, half, 1 - half)

    def overlaps(dest):
        return diag_row // 2 == dest

    def lookup(child, source, slot):
        found = jnp.int32(0)
        count = jnp.int32(0)
        target = source * window + slot
        for d in range(window - group_blocks + 1):
            k = jnp.clip(slot - d, 0, group_blocks - 1)
            hit = map_ref[child, source * group_blocks + k] == target
            found = jnp.where(hit, k, found)
            count = jnp.where(hit, count_ref[child, source * group_blocks + k], count)
        return found, count

    row_iota = lax.broadcasted_iota(jnp.int32, (block, LANES), 0)

    def masked_rows(slot):
        found, count = lookup(core, group, slot)
        kept = (row_iota < count).astype(jnp.float32).astype(jnp.bfloat16)
        return gen_ref[found] * jnp.concatenate([kept] * (rank // LANES), axis=1)

    def project(child, rows):
        return lax.dot_general(
            coupling_ref[child], rows, (((0,), (1,)), ((), ())),
            preferred_element_type=jnp.float32,
        ).astype(jnp.bfloat16)

    def remote(src, dst, send, recv, to_row, to_col):
        return pltpu.make_async_remote_copy(
            src_ref=src, dst_ref=dst, send_sem=send, recv_sem=recv,
            device_id=(to_row, to_col), device_id_type=MESH,
        )

    def load(src, dst, n):
        return pltpu.make_async_copy(src, dst, load_sem.at[n])

    loads = [
        load(src, dst, n)
        for n, (src, dst) in enumerate((
            (map_hbm, map_ref), (count_hbm, count_ref), (gen_hbm, gen_ref),
            (coupling_hbm, coupling_ref), (diag_hbm, diag_ref),
        ))
    ]
    for copy in loads[:4]:
        copy.start()

    barrier = pltpu.get_barrier_semaphore()
    for k in range(1, row_count):
        pl.semaphore_signal(
            barrier, inc=1, device_id=((row + k) % row_count, col), device_id_type=MESH
        )
    for other in (x_col, z_col):
        pl.semaphore_signal(barrier, inc=1, device_id=(row, other), device_id_type=MESH)

    def far_copy(k, child, source, par, i, dest_row):
        t, start, size = steps[i]
        part = pl.ds(start, size)
        return remote(
            far_rows.at[k - 1, t, part], rows_out.at[source, 2 * t + par, child, part],
            far_send.at[k - 1, i], far_recv.at[k - 1, child, i], dest_row, col,
        )

    def piece_copy(k, source, par, child, i, send, recv, to_col):
        t, start, size = steps[i]
        piece = rows_out.at[source, 2 * t + par, child, pl.ds(start, size)]
        at = (k - 1, child, i)
        return remote(piece, piece, send.at[at], recv.at[at], row, to_col)

    def x_copy(k, source, par, child, i):
        return piece_copy(k, source, par, child, i, x_send, x_recv, x_col)

    def z_copy(k, source, par, child, i):
        return piece_copy(k, source, par, child, i, z_send, z_recv, z_col)

    def xr_copy(k, source, par, child, i):
        return piece_copy(k, source, par, child, i, xr_send, xr_recv, x_col)

    def zr_copy(k, source, par, child, i):
        return piece_copy(k, source, par, child, i, zr_send, zr_recv, z_col)

    def pair_copy(child, m):
        return remote(
            pair_rows.at[m], rows_out.at[group, m, child],
            pair_send.at[m], pair_recv.at[m], pair_row, col,
        )

    def near_copy(child, t):
        piece = cols_out.at[group, t, child]
        return remote(piece, piece, near_send.at[t], near_recv.at[t], pair_row, col)

    def col_copy(k, source, t, dest):
        piece = cols_out.at[source, t, core]
        return remote(
            piece, piece, col_send.at[k - 1, t], col_recv.at[k - 1, t], 2 * dest + core, col
        )

    def fwd_copy(k, source, child, t):
        piece = cols_out.at[source, t, child]
        return remote(piece, piece, fwd_send.at[k - 1, t], fwd_recv.at[k - 1, t], pair_row, col)

    def over_copy(k, source, child, t):
        piece = cols_out.at[source, t, child]
        at = (k - 1, child, t)
        return remote(piece, piece, over_send.at[at], over_recv.at[at], pair_row, col)

    def diag_copy(source, child, t):
        return remote(
            own_diag.at[t], diag_in.at[source, child, t],
            diag_send.at[t], diag_recv.at[source, child, t], diag_row, col,
        )

    far = [(k, (group + k) % groups) for k in range(1, groups)]
    sources = [(k, (group + groups - k) % groups) for k in range(1, groups)]
    par = parity(group)

    for copy in loads[:3]:
        copy.wait()
    loads[4].start()
    for t in range(col_cap):
        for k, dest in far:
            slot = (2 * t + parity(dest)) * row_count + 2 * dest + quarter % 2
            far_rows[k - 1, t] = masked_rows(slot)
        if t == 0:
            pl.semaphore_wait(barrier, row_count + 1)
        for i in range(len(steps)):
            if steps[i][0] == t:
                for k, dest in far:
                    far_copy(k, core, group, parity(dest), i, 2 * dest + quarter % 2).start()

    front_loads = [
        pltpu.make_async_copy(front_hbm.at[a, :, h], front_out.at[a, h], front_sem.at[a, h])
        for a in range(front_out.shape[0]) for h in range(front_out.shape[1])
    ]
    for copy in loads[3:]:
        copy.wait()

    for t in range(col_cap):
        cols_out[group, t, core] = project(core, masked_rows(t * col_count + col))
        near_copy(core, t).start()
        for k, dest in far:
            @pl.when(jnp.logical_not(overlaps(dest)))
            def _():
                col_copy(k, group, t, dest).start()

    row_iota2 = lax.broadcasted_iota(jnp.int32, (block, block), 0)
    col_iota2 = lax.broadcasted_iota(jnp.int32, (block, block), 1)
    edge = jnp.maximum(row_iota2, col_iota2)
    for t in range(col_cap):
        found, count = lookup(core, group, t * col_count + col)
        piece = jnp.where(edge < count, diag_ref[found].astype(jnp.float32), 0.0)
        own_diag[t] = piece.astype(jnp.bfloat16)

        @pl.when(row != diag_row)
        def _():
            diag_copy(group, core, t).start()

        @pl.when(row == diag_row)
        def _():
            diag_in[group, core, t] = own_diag[t]

    for copy in front_loads:
        copy.start()
    for m in range(row_cap):
        pair_rows[m] = masked_rows(m * row_count + pair_row)
        pair_copy(core, m).start()
    for m in range(row_cap):
        rows_out[group, m, core] = masked_rows(m * row_count + row)

    def add_diag(source):
        for t in range(col_cap):
            b = source * col_cap + t
            total = diag_in[source, 0, t].astype(jnp.float32) + diag_in[source, 1, t].astype(jnp.float32)
            spot = pl.ds(b % cols_local, block, stride=cols_local)
            for h in range(block // LANES):
                held = front_out.at[b * ratio + half, h].reshape(block * cols_local, LANES)
                held[spot, :] = held[spot, :] + total[:, h * LANES:(h + 1) * LANES]

    @pl.when(holder)
    def _():
        for i in range(len(steps)):
            for k, source in sources:
                for child in range(2):
                    far_copy(k, child, source, par, i, row).wait_recv()
                    x_copy(k, source, par, child, i).start()
                    z_copy(k, source, par, child, i).start()
        for i in range(middle):
            for k, source in sources:
                for child in range(2):
                    z_copy(k, source, 1 - par, child, i).wait_recv()
                    xr_copy(k, source, 1 - par, child, i).start()

        @pl.when(overlaps(group))
        def _():
            for k, source in sources:
                for t in range(col_cap):
                    for child in range(2):
                        cols_out[source, t, child] = project(
                            child, rows_out[source, 2 * t + par, child]
                        )
                        over_copy(k, source, child, t).start()

    @pl.when(jnp.logical_not(holder))
    def _():
        for i in range(middle, len(steps)):
            for k, source in sources:
                for child in range(2):
                    x_copy(k, source, par, child, i).wait_recv()
                    zr_copy(k, source, par, child, i).start()

    @pl.when(jnp.logical_not(overlaps(group)))
    def _():
        for t in range(col_cap):
            for k, source in sources:
                col_copy(k, source, t, group).wait_recv()
                fwd_copy(k, source, core, t).start()

    for copy in front_loads:
        copy.wait()

    @pl.when(row == diag_row)
    def _():
        for t in range(col_cap):
            diag_copy(group, 1 - core, t).wait_recv()
        add_diag(group)

    for m in range(row_cap):
        pair_copy(1 - core, m).wait_recv()
        pair_copy(core, m).wait_send()
    for t in range(col_cap):
        near_copy(1 - core, t).wait_recv()
        near_copy(core, t).wait_send()
    for k, dest in far:
        for i in range(len(steps)):
            far_copy(k, core, group, 0, i, row).wait_send()

    @pl.when(row == diag_row)
    def _():
        for k, source in sources:
            for child in range(2):
                for t in range(col_cap):
                    diag_copy(source, child, t).wait_recv()
            add_diag(source)

    @pl.when(row != diag_row)
    def _():
        for t in range(col_cap):
            diag_copy(group, core, t).wait_send()

    for k, dest in far:
        @pl.when(jnp.logical_not(overlaps(dest)))
        def _():
            for t in range(col_cap):
                col_copy(k, group, t, dest).wait_send()

    @pl.when(holder)
    def _():
        for k, source in sources:
            for child in range(2):
                for i in range(len(steps)):
                    if i >= middle:
                        z_copy(k, source, 1 - par, child, i).wait_recv()
                    else:
                        xr_copy(k, source, 1 - par, child, i).wait_send()
                    x_copy(k, source, par, child, i).wait_send()
                    z_copy(k, source, par, child, i).wait_send()

    @pl.when(jnp.logical_not(holder))
    def _():
        for k, source in sources:
            for child in range(2):
                for i in range(len(steps)):
                    if i >= middle:
                        zr_copy(k, source, par, child, i).wait_send()
                        zr_copy(k, source, 1 - par, child, i).wait_recv()
                    else:
                        x_copy(k, source, par, child, i).wait_recv()
                        xr_copy(k, source, 1 - par, child, i).wait_recv()

    @pl.when(overlaps(group))
    def _():
        @pl.when(holder)
        def _():
            for k, source in sources:
                for t in range(col_cap):
                    for child in range(2):
                        over_copy(k, source, child, t).wait_send()

        @pl.when(jnp.logical_not(holder))
        def _():
            for k, source in sources:
                for t in range(col_cap):
                    for child in range(2):
                        over_copy(k, source, child, t).wait_recv()

    @pl.when(jnp.logical_not(overlaps(group)))
    def _():
        for t in range(col_cap):
            for k, source in sources:
                fwd_copy(k, source, 1 - core, t).wait_recv()
                fwd_copy(k, source, core, t).wait_send()


def add_kernel(
    front_ref, rows_ref, cols_ref, out_ref, staged, out_sem
):
    rows_local, halves, block, cols_local, _ = front_ref.shape
    _, row_cap, _, _, rank = rows_ref.shape
    col_cap = cols_ref.shape[1]

    def write(a, h):
        return pltpu.make_async_copy(staged.at[a, h], out_ref.at[a, :, h], out_sem.at[a, h])

    for a in range(rows_local):
        s, m = divmod(a, row_cap)
        rows = jnp.concatenate([rows_ref[s, m, 0], rows_ref[s, m, 1]], axis=1)
        for b in range(cols_local):
            cols = cols_ref[b // col_cap, b % col_cap].reshape(2 * rank, block)
            tile = jnp.dot(rows, cols, preferred_element_type=jnp.float32)
            spot = pl.ds(b, block, stride=cols_local)
            for h in range(halves):
                src = front_ref.at[a, h].reshape(block * cols_local, LANES)
                dst = staged.at[a, h].reshape(block * cols_local, LANES)
                dst[spot, :] = src[spot, :] + tile[:, h * LANES:(h + 1) * LANES]

        for h in range(halves):
            write(a, h).start()
    for a in range(rows_local):
        for h in range(halves):
            write(a, h).wait()


def shards(parent_front, generators, diagonal_blocks, coupling, block_map, valid_rows):
    row_count = lax.axis_size("row")
    col_count = lax.axis_size("col")
    groups = row_count // 2
    block, rank = generators.shape[1:]
    rows_local = parent_front.shape[0]
    cols_local = parent_front.shape[2]
    row_cap = rows_local // groups
    col_cap = cols_local // groups
    vmem = pl.BlockSpec(memory_space=pltpu.VMEM)
    hbm = pl.BlockSpec(memory_space=pltpu.HBM)
    dma = pltpu.SemaphoreType.DMA
    halves = block // LANES
    split = parent_front.reshape(rows_local, block, cols_local, halves, LANES)
    split = split.transpose(0, 1, 3, 2, 4)
    held = (rows_local, halves, block, cols_local, LANES)
    operands = [
        pltpu.with_memory_space_constraint(x, pltpu.HBM)
        for x in (generators, diagonal_blocks, coupling, block_map, valid_rows, split)
    ]
    far = groups - 1
    pieces = (far, 2, len(steps_of(col_cap, block)))
    rows, cols, front = pl.pallas_call(
        functools.partial(exchange_kernel, row_count, col_count, row_cap, col_cap),
        out_shape=(
            pltpu.VMEM((groups, row_cap, 2, block, rank), jnp.bfloat16),
            pltpu.VMEM((groups, col_cap, 2, rank, block), jnp.bfloat16),
            pltpu.VMEM(held, jnp.float32),
        ),
        in_specs=[hbm] * 6,
        out_specs=(vmem,) * 3,
        scratch_shapes=[
            pltpu.VMEM(generators.shape, jnp.bfloat16),
            pltpu.VMEM(diagonal_blocks.shape, jnp.bfloat16),
            pltpu.VMEM(coupling.shape, jnp.bfloat16),
            pltpu.SMEM(block_map.shape, jnp.int32),
            pltpu.SMEM(valid_rows.shape, jnp.int32),
            dma((5,)),
            dma((rows_local, halves)),
            pltpu.VMEM((far, col_cap, block, rank), jnp.bfloat16),
            pltpu.VMEM((row_cap, block, rank), jnp.bfloat16),
            pltpu.VMEM((col_cap, block, block), jnp.bfloat16),
            pltpu.VMEM((groups, 2, col_cap, block, block), jnp.bfloat16),
            dma((far, len(steps_of(col_cap, block)))),
            dma(pieces),
            dma(pieces),
            dma(pieces),
            dma(pieces),
            dma(pieces),
            dma(pieces),
            dma(pieces),
            dma(pieces),
            dma(pieces),
            dma((row_cap,)),
            dma((row_cap,)),
            dma((col_cap,)),
            dma((col_cap,)),
            dma((far, col_cap)),
            dma((far, col_cap)),
            dma((far, col_cap)),
            dma((far, col_cap)),
            dma((far, 2, col_cap)),
            dma((far, 2, col_cap)),
            dma((col_cap,)),
            dma((groups, 2, col_cap)),
        ],
        compiler_params=pltpu.CompilerParams(
            collective_id=0, has_side_effects=True, vmem_limit_bytes=32 * 1024 * 1024
        ),
    )(*operands)
    out = pl.pallas_call(
        add_kernel,
        out_shape=jax.ShapeDtypeStruct(split.shape, jnp.float32),
        in_specs=[vmem] * 3,
        out_specs=hbm,
        scratch_shapes=[pltpu.VMEM(held, jnp.float32), dma((rows_local, halves))],
        compiler_params=pltpu.CompilerParams(vmem_limit_bytes=32 * 1024 * 1024),
    )(*(pltpu.with_memory_space_constraint(x, pltpu.VMEM) for x in (front, rows, cols)))
    return out.transpose(0, 1, 3, 2, 4).reshape(parent_front.shape)


def solution(mesh):
    in_specs = (
        P(None, "row", None, "col"),
        P("row", None, None),
        P("row", None, None),
        P(),
        P(),
        P(),
    )
    out_specs = P(None, "row", None, "col")
    return jax.shard_map(shards, mesh=mesh, in_specs=in_specs, out_specs=out_specs, check_vma=False)
```

```python
import functools

import jax
import jax.numpy as jnp
from jax import lax
from jax.experimental import pallas as pl
from jax.experimental.pallas import tpu as pltpu
from jax.sharding import PartitionSpec as P

MESH = pl.DeviceIdType.MESH
QUAD = 4
LANES = 128


def steps_of(col_cap, block):
    per_block = QUAD // col_cap
    size = block // per_block
    return [(t, p * size, size) for t in range(col_cap) for p in range(per_block)]


def exchange_kernel(
    row_count, col_count, row_cap, col_cap,
    gen_hbm, diag_hbm, coupling_hbm, map_hbm, count_hbm, front_hbm,
    rows_out, cols_out, front_out,
    gen_ref, diag_ref, coupling_ref, map_ref, count_ref, load_sem, front_sem,
    far_rows, pair_rows, own_diag, diag_in,
    far_send, far_recv, x_send, z_send, step_recv, relay_send, relay_recv,
    pair_send, pair_recv, near_send, near_recv, col_send, col_recv, side_send, side_recv,
    diag_send, diag_recv,
):
    groups = row_count // 2
    group_blocks, block, rank = gen_ref.shape
    window = row_cap * row_count
    steps = steps_of(col_cap, block)
    middle = len(steps) // 2
    ratio = col_count // row_count
    cols_local = groups * col_cap
    row = lax.axis_index("row")
    col = lax.axis_index("col")
    group = row // 2
    core = row % 2
    quarter = col % QUAD
    half = col // row_count
    pair_row = group * 2 + 1 - core
    diag_row = col % row_count
    x_col = col + 1 - 2 * (quarter % 2)
    z_col = col + 2 - 4 * (quarter // 2)
    holder = quarter % 2 == core

    def parity(dest):
        return jnp.where(quarter // 2 == dest % 2, half, 1 - half)

    def overlaps(dest):
        return diag_row // 2 == dest

    def lookup(child, source, slot):
        found = jnp.int32(0)
        count = jnp.int32(0)
        target = source * window + slot
        for d in range(window - group_blocks + 1):
            k = jnp.clip(slot - d, 0, group_blocks - 1)
            hit = map_ref[child, source * group_blocks + k] == target
            found = jnp.where(hit, k, found)
            count = jnp.where(hit, count_ref[child, source * group_blocks + k], count)
        return found, count

    row_iota = lax.broadcasted_iota(jnp.int32, (block, LANES), 0)

    def masked_rows(slot):
        found, count = lookup(core, group, slot)
        kept = (row_iota < count).astype(jnp.float32).astype(jnp.bfloat16)
        return gen_ref[found] * jnp.concatenate([kept] * (rank // LANES), axis=1)

    def project(child, rows):
        return lax.dot_general(
            coupling_ref[child], rows, (((0,), (1,)), ((), ())),
            preferred_element_type=jnp.float32,
        ).astype(jnp.bfloat16)

    def remote(src, dst, send, recv, to_row, to_col):
        return pltpu.make_async_remote_copy(
            src_ref=src, dst_ref=dst, send_sem=send, recv_sem=recv,
            device_id=(to_row, to_col), device_id_type=MESH,
        )

    def load(src, dst, n):
        return pltpu.make_async_copy(src, dst, load_sem.at[n])

    loads = [
        load(src, dst, n)
        for n, (src, dst) in enumerate((
            (map_hbm, map_ref), (count_hbm, count_ref), (gen_hbm, gen_ref),
            (coupling_hbm, coupling_ref), (diag_hbm, diag_ref),
        ))
    ]
    for copy in loads[:4]:
        copy.start()

    barrier = pltpu.get_barrier_semaphore()
    for k in range(1, row_count):
        pl.semaphore_signal(
            barrier, inc=1, device_id=((row + k) % row_count, col), device_id_type=MESH
        )
    for other in (x_col, z_col):
        pl.semaphore_signal(barrier, inc=1, device_id=(row, other), device_id_type=MESH)

    def far_copy(k, child, source, par, i, dest_row):
        t, start, size = steps[i]
        part = pl.ds(start, size)
        return remote(
            far_rows.at[k - 1, t, part], rows_out.at[source, 2 * t + par, child, part],
            far_send.at[k - 1], far_recv.at[k - 1, i], dest_row, col,
        )

    def piece_copy(source, par, i, send, recv, to_col):
        t, start, size = steps[i]
        piece = rows_out.at[source, 2 * t + par, :, pl.ds(start, size)]
        return remote(piece, piece, send, recv, row, to_col)

    def far_landed(k, source, par, i):
        return piece_copy(source, par, i, far_send.at[k - 1], far_recv.at[k - 1, i], col)

    def x_copy(k, source, par, i):
        return piece_copy(source, par, i, x_send.at[k - 1], step_recv.at[k - 1, i], x_col)

    def z_copy(k, source, par, i):
        return piece_copy(source, par, i, z_send.at[k - 1], step_recv.at[k - 1, i], z_col)

    def xr_copy(k, source, par, i):
        return piece_copy(source, par, i, relay_send.at[k - 1], relay_recv.at[k - 1], x_col)

    def zr_copy(k, source, par, i):
        return piece_copy(source, par, i, relay_send.at[k - 1], relay_recv.at[k - 1], z_col)

    def all_of(ref, send, recv):
        return remote(ref, ref, send, recv, pair_row, col)

    def pair_copy(child, m):
        return remote(
            pair_rows.at[m], rows_out.at[group, m, child], pair_send, pair_recv, pair_row, col
        )

    def near_copy(child, t):
        piece = cols_out.at[group, t, child]
        return remote(piece, piece, near_send, near_recv, pair_row, col)

    def col_copy(k, source, t, dest):
        piece = cols_out.at[source, t, core]
        return remote(
            piece, piece, col_send.at[k - 1], col_recv.at[k - 1, t], 2 * dest + core, col
        )

    def fwd_copy(k, source, t):
        piece = cols_out.at[source, t, core]
        return remote(piece, piece, side_send.at[k - 1], side_recv.at[k - 1], pair_row, col)

    def over_copy(k, source, t):
        piece = cols_out.at[source, t]
        return remote(piece, piece, side_send.at[k - 1], side_recv.at[k - 1], pair_row, col)

    def diag_copy(t):
        return remote(
            own_diag.at[t], diag_in.at[group, core, t], diag_send, diag_recv.at[group],
            diag_row, col,
        )

    far = [(k, (group + k) % groups) for k in range(1, groups)]
    sources = [(k, (group + groups - k) % groups) for k in range(1, groups)]
    par = parity(group)

    for copy in loads[:3]:
        copy.wait()
    loads[4].start()
    for t in range(col_cap):
        for k, dest in far:
            slot = (2 * t + parity(dest)) * row_count + 2 * dest + quarter % 2
            far_rows[k - 1, t] = masked_rows(slot)
        if t == 0:
            pl.semaphore_wait(barrier, row_count + 1)
        for i in range(len(steps)):
            if steps[i][0] == t:
                for k, dest in far:
                    far_copy(k, core, group, parity(dest), i, 2 * dest + quarter % 2).start()

    front_loads = [
        pltpu.make_async_copy(front_hbm.at[:, :, h], front_out.at[:, h], front_sem.at[h])
        for h in range(front_out.shape[1])
    ]
    for copy in loads[3:]:
        copy.wait()

    for t in range(col_cap):
        cols_out[group, t, core] = project(core, masked_rows(t * col_count + col))
        near_copy(core, t).start()
        for k, dest in far:
            @pl.when(jnp.logical_not(overlaps(dest)))
            def _():
                col_copy(k, group, t, dest).start()

    row_iota2 = lax.broadcasted_iota(jnp.int32, (block, block), 0)
    col_iota2 = lax.broadcasted_iota(jnp.int32, (block, block), 1)
    edge = jnp.maximum(row_iota2, col_iota2)
    for t in range(col_cap):
        found, count = lookup(core, group, t * col_count + col)
        piece = jnp.where(edge < count, diag_ref[found].astype(jnp.float32), 0.0)
        own_diag[t] = piece.astype(jnp.bfloat16)

        @pl.when(row != diag_row)
        def _():
            diag_copy(t).start()

        @pl.when(row == diag_row)
        def _():
            diag_in[group, core, t] = own_diag[t]

    for copy in front_loads:
        copy.start()
    for m in range(row_cap):
        pair_rows[m] = masked_rows(m * row_count + pair_row)
        pair_copy(core, m).start()
    for m in range(row_cap):
        rows_out[group, m, core] = masked_rows(m * row_count + row)

    def add_diag(source):
        for t in range(col_cap):
            b = source * col_cap + t
            total = diag_in[source, 0, t].astype(jnp.float32) + diag_in[source, 1, t].astype(jnp.float32)
            spot = pl.ds(b % cols_local, block, stride=cols_local)
            for h in range(block // LANES):
                held = front_out.at[b * ratio + half, h].reshape(block * cols_local, LANES)
                held[spot, :] = held[spot, :] + total[:, h * LANES:(h + 1) * LANES]

    @pl.when(holder)
    def _():
        for i in range(len(steps)):
            for k, source in sources:
                far_landed(k, source, par, i).wait_recv()
                x_copy(k, source, par, i).start()
                z_copy(k, source, par, i).start()
        for i in range(middle):
            for k, source in sources:
                z_copy(k, source, 1 - par, i).wait_recv()
                xr_copy(k, source, 1 - par, i).start()

        @pl.when(overlaps(group))
        def _():
            for k, source in sources:
                for t in range(col_cap):
                    for child in range(2):
                        cols_out[source, t, child] = project(
                            child, rows_out[source, 2 * t + par, child]
                        )
                    over_copy(k, source, t).start()

    @pl.when(jnp.logical_not(holder))
    def _():
        for i in range(middle, len(steps)):
            for k, source in sources:
                x_copy(k, source, par, i).wait_recv()
                zr_copy(k, source, par, i).start()

    @pl.when(jnp.logical_not(overlaps(group)))
    def _():
        for t in range(col_cap):
            for k, source in sources:
                col_copy(k, source, t, group).wait_recv()
                fwd_copy(k, source, t).start()

    for copy in front_loads:
        copy.wait()

    @pl.when(row == diag_row)
    def _():
        all_of(diag_in.at[group, 1 - core], diag_send, diag_recv.at[group]).wait_recv()
        add_diag(group)

    all_of(pair_rows, pair_send, pair_recv).wait_recv()
    all_of(pair_rows, pair_send, pair_recv).wait_send()
    all_of(cols_out.at[group, :, 1 - core], near_send, near_recv).wait_recv()
    all_of(cols_out.at[group, :, core], near_send, near_recv).wait_send()
    for k, dest in far:
        all_of(far_rows.at[k - 1], far_send.at[k - 1], relay_recv.at[k - 1]).wait_send()

    @pl.when(row != diag_row)
    def _():
        all_of(own_diag, diag_send, diag_recv.at[group]).wait_send()

    for k, dest in far:
        @pl.when(jnp.logical_not(overlaps(dest)))
        def _():
            all_of(cols_out.at[group, :, core], col_send.at[k - 1], side_recv.at[k - 1]).wait_send()

    @pl.when(row == diag_row)
    def _():
        for k, source in sources:
            all_of(diag_in.at[source], diag_send, diag_recv.at[source]).wait_recv()
            add_diag(source)

    one_part = rows_out.at[group, pl.ds(0, col_cap)]
    half_part = rows_out.at[group, pl.ds(0, col_cap), 0]

    @pl.when(holder)
    def _():
        for k, source in sources:
            for i in range(middle, len(steps)):
                z_copy(k, source, 1 - par, i).wait_recv()
            all_of(one_part, x_send.at[k - 1], relay_recv.at[k - 1]).wait_send()
            all_of(one_part, z_send.at[k - 1], relay_recv.at[k - 1]).wait_send()
            all_of(half_part, relay_send.at[k - 1], relay_recv.at[k - 1]).wait_send()

    @pl.when(jnp.logical_not(holder))
    def _():
        for k, source in sources:
            for i in range(middle):
                x_copy(k, source, par, i).wait_recv()
            all_of(half_part, relay_send.at[k - 1], relay_recv.at[k - 1]).wait_send()
            all_of(one_part, relay_send.at[k - 1], relay_recv.at[k - 1]).wait_recv()

    @pl.when(overlaps(group))
    def _():
        for k, source in sources:
            moved = all_of(cols_out.at[source], side_send.at[k - 1], side_recv.at[k - 1])

            @pl.when(holder)
            def _():
                moved.wait_send()

            @pl.when(jnp.logical_not(holder))
            def _():
                moved.wait_recv()

    @pl.when(jnp.logical_not(overlaps(group)))
    def _():
        for k, source in sources:
            moved = all_of(cols_out.at[source, :, core], side_send.at[k - 1], side_recv.at[k - 1])
            moved.wait_recv()
            moved.wait_send()


def add_kernel(
    front_ref, rows_ref, cols_ref, out_ref, staged, out_sem
):
    rows_local, halves, block, cols_local, _ = front_ref.shape
    _, row_cap, _, _, rank = rows_ref.shape
    col_cap = cols_ref.shape[1]

    def write(a, h):
        return pltpu.make_async_copy(staged.at[a, h], out_ref.at[a, :, h], out_sem)

    for a in range(rows_local):
        s, m = divmod(a, row_cap)
        rows = jnp.concatenate([rows_ref[s, m, 0], rows_ref[s, m, 1]], axis=1)
        for b in range(cols_local):
            cols = cols_ref[b // col_cap, b % col_cap].reshape(2 * rank, block)
            tile = jnp.dot(rows, cols, preferred_element_type=jnp.float32)
            spot = pl.ds(b, block, stride=cols_local)
            for h in range(halves):
                src = front_ref.at[a, h].reshape(block * cols_local, LANES)
                dst = staged.at[a, h].reshape(block * cols_local, LANES)
                dst[spot, :] = src[spot, :] + tile[:, h * LANES:(h + 1) * LANES]

        for h in range(halves):
            write(a, h).start()
    pltpu.make_async_copy(staged, staged, out_sem).wait()


def shards(parent_front, generators, diagonal_blocks, coupling, block_map, valid_rows):
    row_count = lax.axis_size("row")
    col_count = lax.axis_size("col")
    groups = row_count // 2
    block, rank = generators.shape[1:]
    rows_local = parent_front.shape[0]
    cols_local = parent_front.shape[2]
    row_cap = rows_local // groups
    col_cap = cols_local // groups
    vmem = pl.BlockSpec(memory_space=pltpu.VMEM)
    hbm = pl.BlockSpec(memory_space=pltpu.HBM)
    dma = pltpu.SemaphoreType.DMA
    halves = block // LANES
    split = parent_front.reshape(rows_local, block, cols_local, halves, LANES)
    split = split.transpose(0, 1, 3, 2, 4)
    held = (rows_local, halves, block, cols_local, LANES)
    operands = [
        pltpu.with_memory_space_constraint(x, pltpu.HBM)
        for x in (generators, diagonal_blocks, coupling, block_map, valid_rows, split)
    ]
    far = groups - 1
    rows, cols, front = pl.pallas_call(
        functools.partial(exchange_kernel, row_count, col_count, row_cap, col_cap),
        out_shape=(
            pltpu.VMEM((groups, row_cap, 2, block, rank), jnp.bfloat16),
            pltpu.VMEM((groups, col_cap, 2, rank, block), jnp.bfloat16),
            pltpu.VMEM(held, jnp.float32),
        ),
        in_specs=[hbm] * 6,
        out_specs=(vmem,) * 3,
        scratch_shapes=[
            pltpu.VMEM(generators.shape, jnp.bfloat16),
            pltpu.VMEM(diagonal_blocks.shape, jnp.bfloat16),
            pltpu.VMEM(coupling.shape, jnp.bfloat16),
            pltpu.SMEM(block_map.shape, jnp.int32),
            pltpu.SMEM(valid_rows.shape, jnp.int32),
            dma((5,)),
            dma((halves,)),
            pltpu.VMEM((far, col_cap, block, rank), jnp.bfloat16),
            pltpu.VMEM((row_cap, block, rank), jnp.bfloat16),
            pltpu.VMEM((col_cap, block, block), jnp.bfloat16),
            pltpu.VMEM((groups, 2, col_cap, block, block), jnp.bfloat16),
            dma((far,)),
            dma((far, QUAD)),
            dma((far,)),
            dma((far,)),
            dma((far, QUAD)),
            dma((far,)),
            dma((far,)),
            dma,
            dma,
            dma,
            dma,
            dma((far,)),
            dma((far, col_cap)),
            dma((far,)),
            dma((far,)),
            dma,
            dma((groups,)),
        ],
        compiler_params=pltpu.CompilerParams(
            collective_id=0, has_side_effects=True, vmem_limit_bytes=32 * 1024 * 1024
        ),
    )(*operands)
    out = pl.pallas_call(
        add_kernel,
        out_shape=jax.ShapeDtypeStruct(split.shape, jnp.float32),
        in_specs=[vmem] * 3,
        out_specs=hbm,
        scratch_shapes=[pltpu.VMEM(held, jnp.float32), dma],
        compiler_params=pltpu.CompilerParams(vmem_limit_bytes=32 * 1024 * 1024),
    )(*(pltpu.with_memory_space_constraint(x, pltpu.VMEM) for x in (front, rows, cols)))
    return out.transpose(0, 1, 3, 2, 4).reshape(parent_front.shape)


def solution(mesh):
    in_specs = (
        P(None, "row", None, "col"),
        P("row", None, None),
        P("row", None, None),
        P(),
        P(),
        P(),
    )
    out_specs = P(None, "row", None, "col")
    return jax.shard_map(shards, mesh=mesh, in_specs=in_specs, out_specs=out_specs, check_vma=False)
```

```python
import functools

import jax
import jax.numpy as jnp
from jax import lax
from jax.experimental import pallas as pl
from jax.experimental.pallas import tpu as pltpu
from jax.sharding import PartitionSpec as P

MESH = pl.DeviceIdType.MESH
QUAD = 4
STEPS = 16
LANES = 128


def steps_of(col_cap, block):
    per_block = STEPS // col_cap
    size = block // per_block
    return [(t, p * size, size) for t in range(col_cap) for p in range(per_block)]


def exchange_kernel(
    row_count, col_count, row_cap, col_cap,
    gen_hbm, diag_hbm, coupling_hbm, map_hbm, count_hbm, front_hbm,
    rows_out, cols_out, front_out,
    gen_ref, diag_ref, coupling_ref, map_ref, count_ref, load_sem, front_sem,
    far_rows, extra_rows, pair_rows, own_diag, swap_diag, sum_diag, diag_in,
    far_send, far_recv, x_send, z_send, step_recv, relay_send, relay_recv,
    pair_send, pair_recv, near_send, near_recv, col_send, col_recv, side_send, side_recv,
    swap_send, swap_recv, diag_send, diag_recv, extra_send, extra_recv,
):
    groups = row_count // 2
    group_blocks, block, rank = gen_ref.shape
    window = row_cap * row_count
    steps = steps_of(col_cap, block)
    middle = len(steps) // 2
    first = middle // 2
    part_rows = col_cap * block // 2
    if col_cap == 1:
        extras = [(0, part_rows, part_rows)]
    else:
        extras = [(t, 0, block) for t in range(col_cap // 2, col_cap)]
    ratio = col_count // row_count
    cols_local = groups * col_cap
    row = lax.axis_index("row")
    col = lax.axis_index("col")
    group = row // 2
    core = row % 2
    quarter = col % QUAD
    half = col // row_count
    pair_row = group * 2 + 1 - core
    diag_row = col % row_count
    x_col = col + 1 - 2 * (quarter % 2)
    z_col = col + 2 - 4 * (quarter // 2)
    holder = quarter % 2 == core

    def parity(dest):
        return jnp.where(quarter // 2 == dest % 2, half, 1 - half)

    def overlaps(dest):
        return diag_row // 2 == dest

    z_over = (z_col % row_count) // 2 == group

    def lookup(child, source, slot):
        found = jnp.int32(0)
        count = jnp.int32(0)
        target = source * window + slot
        for d in range(window - group_blocks + 1):
            k = jnp.clip(slot - d, 0, group_blocks - 1)
            hit = map_ref[child, source * group_blocks + k] == target
            found = jnp.where(hit, k, found)
            count = jnp.where(hit, count_ref[child, source * group_blocks + k], count)
        return found, count

    row_iota = lax.broadcasted_iota(jnp.int32, (block, LANES), 0)

    def masked_rows(slot):
        found, count = lookup(core, group, slot)
        kept = (row_iota < count).astype(jnp.float32).astype(jnp.bfloat16)
        return gen_ref[found] * jnp.concatenate([kept] * (rank // LANES), axis=1)

    def project(child, rows):
        return lax.dot_general(
            coupling_ref[child], rows, (((0,), (1,)), ((), ())),
            preferred_element_type=jnp.float32,
        ).astype(jnp.bfloat16)

    def remote(src, dst, send, recv, to_row, to_col):
        return pltpu.make_async_remote_copy(
            src_ref=src, dst_ref=dst, send_sem=send, recv_sem=recv,
            device_id=(to_row, to_col), device_id_type=MESH,
        )

    def load(src, dst, n):
        return pltpu.make_async_copy(src, dst, load_sem.at[n])

    loads = [
        load(src, dst, n)
        for n, (src, dst) in enumerate((
            (map_hbm, map_ref), (count_hbm, count_ref), (gen_hbm, gen_ref),
            (coupling_hbm, coupling_ref), (diag_hbm, diag_ref),
        ))
    ]
    for copy in loads[:4]:
        copy.start()

    barrier = pltpu.get_barrier_semaphore()
    for k in range(1, row_count):
        pl.semaphore_signal(
            barrier, inc=1, device_id=((row + k) % row_count, col), device_id_type=MESH
        )
    for other in (x_col, z_col):
        pl.semaphore_signal(barrier, inc=1, device_id=(row, other), device_id_type=MESH)

    def far_copy(k, child, source, par, i, dest_row):
        t, start, size = steps[i]
        part = pl.ds(start, size)
        return remote(
            far_rows.at[k - 1, t, part], rows_out.at[source, 2 * t + par, child, part],
            far_send.at[k - 1], far_recv.at[k - 1, i], dest_row, col,
        )

    def piece_copy(source, par, i, send, recv, to_col):
        t, start, size = steps[i]
        piece = rows_out.at[source, 2 * t + par, :, pl.ds(start, size)]
        return remote(piece, piece, send, recv, row, to_col)

    def far_landed(k, source, par, i):
        return piece_copy(source, par, i, far_send.at[k - 1], far_recv.at[k - 1, i], col)

    def x_copy(k, source, par, i):
        return piece_copy(source, par, i, x_send.at[k - 1], step_recv.at[k - 1, i], x_col)

    def z_copy(k, source, par, i):
        return piece_copy(source, par, i, z_send.at[k - 1], step_recv.at[k - 1, i], z_col)

    def xr_copy(k, source, par, i):
        return piece_copy(source, par, i, relay_send.at[k - 1], relay_recv.at[k - 1], x_col)

    def zr_copy(k, source, par, i):
        return piece_copy(source, par, i, relay_send.at[k - 1], relay_recv.at[k - 1], z_col)

    def all_of(ref, send, recv):
        return remote(ref, ref, send, recv, pair_row, col)

    def pair_copy(child, m):
        return remote(
            pair_rows.at[m], rows_out.at[group, m, child], pair_send, pair_recv, pair_row, col
        )

    def near_copy(child, t):
        piece = cols_out.at[group, t, child]
        return remote(piece, piece, near_send, near_recv, pair_row, col)

    def col_copy(k, source, t, dest):
        piece = cols_out.at[source, t, core]
        return remote(
            piece, piece, col_send.at[k - 1], col_recv.at[k - 1, t], 2 * dest + core, col
        )

    def fwd_copy(k, source, t):
        piece = cols_out.at[source, t, core]
        return remote(piece, piece, side_send.at[k - 1], side_recv.at[k - 1], pair_row, col)

    def over_copy(k, source, t):
        piece = cols_out.at[source, t]
        return remote(piece, piece, side_send.at[k - 1], side_recv.at[k - 1], pair_row, col)

    def swap_copy():
        return remote(
            own_diag.at[pl.ds((1 - core) * part_rows, part_rows)], swap_diag,
            swap_send, swap_recv, pair_row, col,
        )

    def diag_copy():
        return remote(
            sum_diag, diag_in.at[group, pl.ds(core * part_rows, part_rows)],
            diag_send, diag_recv.at[group], diag_row, col,
        )

    far = [(k, (group + k) % groups) for k in range(1, groups)]
    sources = [(k, (group + groups - k) % groups) for k in range(1, groups)]
    par = parity(group)

    for copy in loads[:3]:
        copy.wait()
    loads[4].start()
    for t in range(col_cap):
        for k, dest in far:
            slot = (2 * t + parity(dest)) * row_count + 2 * dest + quarter % 2
            far_rows[k - 1, t] = masked_rows(slot)
        if t == 0:
            pl.semaphore_wait(barrier, row_count + 1)
        for i in range(len(steps)):
            if steps[i][0] == t:
                for k, dest in far:
                    far_copy(k, core, group, parity(dest), i, 2 * dest + quarter % 2).start()
    for k, dest in far:
        @pl.when(overlaps(dest))
        def _():
            for n, (t, start, size) in enumerate(extras):
                slot = (2 * t + 1 - parity(dest)) * row_count + 2 * dest + 1 - quarter % 2
                extra_rows[n] = masked_rows(slot)[start:start + size]
                copy = remote(
                    extra_rows.at[n],
                    rows_out.at[group, 2 * t + 1 - parity(dest), core, pl.ds(start, size)],
                    extra_send, extra_recv.at[k - 1], 2 * dest + 1 - quarter % 2, col,
                )
                copy.start()

    front_loads = [
        pltpu.make_async_copy(front_hbm.at[:, :, h], front_out.at[:, h], front_sem.at[h])
        for h in range(front_out.shape[1])
    ]
    for copy in loads[3:]:
        copy.wait()

    for t in range(col_cap):
        cols_out[group, t, core] = project(core, masked_rows(t * col_count + col))
        near_copy(core, t).start()
        for k, dest in far:
            @pl.when(jnp.logical_not(overlaps(dest)))
            def _():
                col_copy(k, group, t, dest).start()

    row_iota2 = lax.broadcasted_iota(jnp.int32, (block, block), 0)
    col_iota2 = lax.broadcasted_iota(jnp.int32, (block, block), 1)
    edge = jnp.maximum(row_iota2, col_iota2)
    for t in range(col_cap):
        found, count = lookup(core, group, t * col_count + col)
        piece = jnp.where(edge < count, diag_ref[found].astype(jnp.float32), 0.0)
        own_diag[t * block:(t + 1) * block, :] = piece.astype(jnp.bfloat16)
    swap_copy().start()

    def send_diag():
        swap_copy().wait_recv()
        own = own_diag[pl.ds(core * part_rows, part_rows), :].astype(jnp.float32)
        total = (own + swap_diag[...].astype(jnp.float32)).astype(jnp.bfloat16)

        @pl.when(row != diag_row)
        def _():
            sum_diag[...] = total
            diag_copy().start()

        @pl.when(row == diag_row)
        def _():
            diag_in[group, pl.ds(core * part_rows, part_rows), :] = total

    for copy in front_loads:
        copy.start()
    for m in range(row_cap):
        pair_rows[m] = masked_rows(m * row_count + pair_row)
        pair_copy(core, m).start()
    for m in range(row_cap):
        rows_out[group, m, core] = masked_rows(m * row_count + row)

    def add_diag(source):
        for t in range(col_cap):
            b = source * col_cap + t
            total = diag_in[source, t * block:(t + 1) * block, :].astype(jnp.float32)
            spot = pl.ds(b % cols_local, block, stride=cols_local)
            for h in range(block // LANES):
                held = front_out.at[b * ratio + half, h].reshape(block * cols_local, LANES)
                held[spot, :] = held[spot, :] + total[:, h * LANES:(h + 1) * LANES]

    def relay_x(count):
        for i in range(count):
            for k, source in sources:
                z_copy(k, source, 1 - par, i).wait_recv()
                xr_copy(k, source, 1 - par, i).start()

    def relay_z(low, high):
        for i in range(low, high):
            for k, source in sources:
                x_copy(k, source, par, i).wait_recv()
                zr_copy(k, source, par, i).start()

    @pl.when(holder)
    def _():
        for i in range(len(steps)):
            for k, source in sources:
                far_landed(k, source, par, i).wait_recv()
                x_copy(k, source, par, i).start()
                z_copy(k, source, par, i).start()
            if i == first:
                send_diag()

        @pl.when(overlaps(group))
        def _():
            relay_x(first)

        @pl.when(jnp.logical_not(overlaps(group)))
        def _():
            relay_x(middle)

        @pl.when(overlaps(group))
        def _():
            for k, source in sources:
                for t in range(col_cap):
                    for child in range(2):
                        cols_out[source, t, child] = project(
                            child, rows_out[source, 2 * t + par, child]
                        )
                    over_copy(k, source, t).start()

    @pl.when(jnp.logical_not(holder))
    def _():
        send_diag()

        @pl.when(z_over)
        def _():
            relay_z(first, middle)

        @pl.when(jnp.logical_not(z_over))
        def _():
            relay_z(middle, len(steps))

    @pl.when(jnp.logical_not(overlaps(group)))
    def _():
        for t in range(col_cap):
            for k, source in sources:
                col_copy(k, source, t, group).wait_recv()
                fwd_copy(k, source, t).start()

    for copy in front_loads:
        copy.wait()

    @pl.when(row == diag_row)
    def _():
        all_of(sum_diag, diag_send, diag_recv.at[group]).wait_recv()
        add_diag(group)

    all_of(pair_rows, pair_send, pair_recv).wait_recv()
    all_of(pair_rows, pair_send, pair_recv).wait_send()
    all_of(cols_out.at[group, :, 1 - core], near_send, near_recv).wait_recv()
    all_of(cols_out.at[group, :, core], near_send, near_recv).wait_send()
    for k, dest in far:
        all_of(far_rows.at[k - 1], far_send.at[k - 1], relay_recv.at[k - 1]).wait_send()

    swap_copy().wait_send()

    @pl.when(row != diag_row)
    def _():
        diag_copy().wait_send()

    for k, dest in far:
        @pl.when(jnp.logical_not(overlaps(dest)))
        def _():
            all_of(cols_out.at[group, :, core], col_send.at[k - 1], side_recv.at[k - 1]).wait_send()

        @pl.when(overlaps(dest))
        def _():
            all_of(extra_rows, extra_send, extra_recv.at[k - 1]).wait_send()

    @pl.when(row == diag_row)
    def _():
        for k, source in sources:
            all_of(diag_in.at[source], diag_send, diag_recv.at[source]).wait_recv()
            add_diag(source)

    one_part = rows_out.at[group, pl.ds(0, col_cap)]
    half_part = rows_out.at[group, pl.ds(0, col_cap), 0]
    low_part = extra_rows

    def moved_part(part, k):
        return all_of(part, relay_send.at[k - 1], relay_recv.at[k - 1])

    @pl.when(holder)
    def _():
        for k, source in sources:
            for i in range(middle, len(steps)):
                z_copy(k, source, 1 - par, i).wait_recv()
            all_of(one_part, x_send.at[k - 1], relay_recv.at[k - 1]).wait_send()
            all_of(one_part, z_send.at[k - 1], relay_recv.at[k - 1]).wait_send()

            @pl.when(overlaps(group))
            def _():
                for i in range(first, middle):
                    z_copy(k, source, 1 - par, i).wait_recv()
                moved_part(low_part, k).wait_send()

            @pl.when(jnp.logical_not(overlaps(group)))
            def _():
                moved_part(half_part, k).wait_send()

    @pl.when(jnp.logical_not(holder))
    def _():
        for k, source in sources:
            for i in range(first):
                x_copy(k, source, par, i).wait_recv()

            @pl.when(z_over)
            def _():
                for i in range(middle, len(steps)):
                    x_copy(k, source, par, i).wait_recv()
                moved_part(low_part, k).wait_send()

            @pl.when(jnp.logical_not(z_over))
            def _():
                for i in range(first, middle):
                    x_copy(k, source, par, i).wait_recv()
                moved_part(half_part, k).wait_send()

            @pl.when(overlaps(group))
            def _():
                all_of(half_part, extra_send, extra_recv.at[k - 1]).wait_recv()
                moved_part(half_part, k).wait_recv()

            @pl.when(jnp.logical_not(overlaps(group)))
            def _():
                moved_part(one_part, k).wait_recv()

    @pl.when(overlaps(group))
    def _():
        for k, source in sources:
            moved = all_of(cols_out.at[source], side_send.at[k - 1], side_recv.at[k - 1])

            @pl.when(holder)
            def _():
                moved.wait_send()

            @pl.when(jnp.logical_not(holder))
            def _():
                moved.wait_recv()

    @pl.when(jnp.logical_not(overlaps(group)))
    def _():
        for k, source in sources:
            moved = all_of(cols_out.at[source, :, core], side_send.at[k - 1], side_recv.at[k - 1])
            moved.wait_recv()
            moved.wait_send()


def add_kernel(
    front_ref, rows_ref, cols_ref, out_ref, staged, out_sem
):
    rows_local, halves, block, cols_local, _ = front_ref.shape
    _, row_cap, _, _, rank = rows_ref.shape
    col_cap = cols_ref.shape[1]

    def write(a, h):
        return pltpu.make_async_copy(staged.at[a, h], out_ref.at[a, :, h], out_sem)

    for a in range(rows_local):
        s, m = divmod(a, row_cap)
        rows = jnp.concatenate([rows_ref[s, m, 0], rows_ref[s, m, 1]], axis=1)
        for b in range(cols_local):
            cols = cols_ref[b // col_cap, b % col_cap].reshape(2 * rank, block)
            tile = jnp.dot(rows, cols, preferred_element_type=jnp.float32)
            spot = pl.ds(b, block, stride=cols_local)
            for h in range(halves):
                src = front_ref.at[a, h].reshape(block * cols_local, LANES)
                dst = staged.at[a, h].reshape(block * cols_local, LANES)
                dst[spot, :] = src[spot, :] + tile[:, h * LANES:(h + 1) * LANES]

        for h in range(halves):
            write(a, h).start()
    pltpu.make_async_copy(staged, staged, out_sem).wait()


def shards(parent_front, generators, diagonal_blocks, coupling, block_map, valid_rows):
    row_count = lax.axis_size("row")
    col_count = lax.axis_size("col")
    groups = row_count // 2
    block, rank = generators.shape[1:]
    rows_local = parent_front.shape[0]
    cols_local = parent_front.shape[2]
    row_cap = rows_local // groups
    col_cap = cols_local // groups
    vmem = pl.BlockSpec(memory_space=pltpu.VMEM)
    hbm = pl.BlockSpec(memory_space=pltpu.HBM)
    dma = pltpu.SemaphoreType.DMA
    halves = block // LANES
    split = parent_front.reshape(rows_local, block, cols_local, halves, LANES)
    split = split.transpose(0, 1, 3, 2, 4)
    held = (rows_local, halves, block, cols_local, LANES)
    operands = [
        pltpu.with_memory_space_constraint(x, pltpu.HBM)
        for x in (generators, diagonal_blocks, coupling, block_map, valid_rows, split)
    ]
    far = groups - 1
    extra = (max(col_cap // 2, 1), block if col_cap > 1 else block // 2, rank)
    rows, cols, front = pl.pallas_call(
        functools.partial(exchange_kernel, row_count, col_count, row_cap, col_cap),
        out_shape=(
            pltpu.VMEM((groups, row_cap, 2, block, rank), jnp.bfloat16),
            pltpu.VMEM((groups, col_cap, 2, rank, block), jnp.bfloat16),
            pltpu.VMEM(held, jnp.float32),
        ),
        in_specs=[hbm] * 6,
        out_specs=(vmem,) * 3,
        scratch_shapes=[
            pltpu.VMEM(generators.shape, jnp.bfloat16),
            pltpu.VMEM(diagonal_blocks.shape, jnp.bfloat16),
            pltpu.VMEM(coupling.shape, jnp.bfloat16),
            pltpu.SMEM(block_map.shape, jnp.int32),
            pltpu.SMEM(valid_rows.shape, jnp.int32),
            dma((5,)),
            dma((halves,)),
            pltpu.VMEM((far, col_cap, block, rank), jnp.bfloat16),
            pltpu.VMEM(extra, jnp.bfloat16),
            pltpu.VMEM((row_cap, block, rank), jnp.bfloat16),
            pltpu.VMEM((col_cap * block, block), jnp.bfloat16),
            pltpu.VMEM((col_cap * block // 2, block), jnp.bfloat16),
            pltpu.VMEM((col_cap * block // 2, block), jnp.bfloat16),
            pltpu.VMEM((groups, col_cap * block, block), jnp.bfloat16),
            dma((far,)),
            dma((far, STEPS)),
            dma((far,)),
            dma((far,)),
            dma((far, STEPS)),
            dma((far,)),
            dma((far,)),
            dma,
            dma,
            dma,
            dma,
            dma((far,)),
            dma((far, col_cap)),
            dma((far,)),
            dma((far,)),
            dma,
            dma,
            dma,
            dma((groups,)),
            dma,
            dma((far,)),
        ],
        compiler_params=pltpu.CompilerParams(
            collective_id=0, has_side_effects=True, vmem_limit_bytes=32 * 1024 * 1024
        ),
    )(*operands)
    out = pl.pallas_call(
        add_kernel,
        out_shape=jax.ShapeDtypeStruct(split.shape, jnp.float32),
        in_specs=[vmem] * 3,
        out_specs=hbm,
        scratch_shapes=[pltpu.VMEM(held, jnp.float32), dma],
        compiler_params=pltpu.CompilerParams(vmem_limit_bytes=32 * 1024 * 1024),
    )(*(pltpu.with_memory_space_constraint(x, pltpu.VMEM) for x in (front, rows, cols)))
    return out.transpose(0, 1, 3, 2, 4).reshape(parent_front.shape)


def solution(mesh):
    in_specs = (
        P(None, "row", None, "col"),
        P("row", None, None),
        P("row", None, None),
        P(),
        P(),
        P(),
    )
    out_specs = P(None, "row", None, "col")
    return jax.shard_map(shards, mesh=mesh, in_specs=in_specs, out_specs=out_specs, check_vma=False)
```

```python
import functools

import jax
import jax.numpy as jnp
from jax import lax
from jax.experimental import pallas as pl
from jax.experimental.pallas import tpu as pltpu
from jax.sharding import PartitionSpec as P

MESH = pl.DeviceIdType.MESH
QUAD = 4
STEPS = 16
LANES = 128


def steps_of(col_cap, block):
    per_block = STEPS // col_cap
    size = block // per_block
    return [(t, p * size, size) for t in range(col_cap) for p in range(per_block)]


def exchange_kernel(
    row_count, col_count, row_cap, col_cap,
    gen_hbm, diag_hbm, coupling_hbm, map_hbm, count_hbm, front_hbm,
    rows_out, cols_out, front_out,
    gen_ref, near_ref, diag_ref, coupling_ref, map_ref, count_ref, load_sem,
    far_rows, extra_rows, pair_rows, own_diag, swap_diag, sum_diag, diag_in,
    far_send, far_recv, x_send, z_send, step_recv, relay_send, relay_recv,
    pair_send, pair_recv, near_send, near_recv, col_send, col_recv, side_send, side_recv,
    swap_send, swap_recv, diag_send, diag_recv, extra_send, extra_recv,
):
    groups = row_count // 2
    group_blocks, block, rank = gen_ref.shape
    window = row_cap * row_count
    steps = steps_of(col_cap, block)
    middle = len(steps) // 2
    first = len(steps) // 4
    last = len(steps) // 2
    part_rows = col_cap * block // 2
    extra_size = col_cap * block // 2
    extra_t, extra_start, _ = steps[last]
    ratio = col_count // row_count
    cols_local = groups * col_cap
    row = lax.axis_index("row")
    col = lax.axis_index("col")
    group = row // 2
    core = row % 2
    quarter = col % QUAD
    half = col // row_count
    pair_row = group * 2 + 1 - core
    diag_row = col % row_count
    x_col = col + 1 - 2 * (quarter % 2)
    z_col = col + 2 - 4 * (quarter // 2)
    holder = quarter % 2 == core

    def parity(dest):
        return jnp.where(quarter // 2 == dest % 2, half, 1 - half)

    def overlaps(dest):
        return diag_row // 2 == dest

    z_over = (z_col % row_count) // 2 == group

    def lookup(child, source, slot):
        found = jnp.int32(0)
        count = jnp.int32(0)
        target = source * window + slot
        for d in range(window - group_blocks + 1):
            k = jnp.clip(slot - d, 0, group_blocks - 1)
            hit = map_ref[child, source * group_blocks + k] == target
            found = jnp.where(hit, k, found)
            count = jnp.where(hit, count_ref[child, source * group_blocks + k], count)
        return found, count

    row_iota = lax.broadcasted_iota(jnp.int32, (block, LANES), 0)

    def masked(rows, count):
        kept = (row_iota < count).astype(jnp.float32).astype(jnp.bfloat16)
        return rows * jnp.concatenate([kept] * (rank // LANES), axis=1)

    def masked_rows(slot):
        found, count = lookup(core, group, slot)
        return masked(gen_ref[found], count)

    def project(child, rows):
        return lax.dot_general(
            coupling_ref[child], rows, (((0,), (1,)), ((), ())),
            preferred_element_type=jnp.float32,
        ).astype(jnp.bfloat16)

    def remote(src, dst, send, recv, to_row, to_col):
        return pltpu.make_async_remote_copy(
            src_ref=src, dst_ref=dst, send_sem=send, recv_sem=recv,
            device_id=(to_row, to_col), device_id_type=MESH,
        )

    def load(src, dst, n):
        return pltpu.make_async_copy(src, dst, load_sem.at[n])

    far = [(k, (group + k) % groups) for k in range(1, groups)]
    sources = [(k, (group + groups - k) % groups) for k in range(1, groups)]
    par = parity(group)
    spread = near_ref.shape[1]

    def far_slot(dest, t):
        return (2 * t + parity(dest)) * row_count + 2 * dest + quarter % 2

    def near_start(dest):
        return jnp.clip(far_slot(dest, 0) - spread + 1, 0, group_blocks - spread)

    map_load = load(map_hbm, map_ref, 0)
    count_load = load(count_hbm, count_ref, 1)
    near_loads = [
        load(gen_hbm.at[pl.ds(near_start(dest), spread)], near_ref.at[k - 1], 2) for k, dest in far
    ]
    gen_load = load(gen_hbm, gen_ref, 3)
    coupling_load = load(coupling_hbm, coupling_ref, 0)
    diag_load = load(diag_hbm, diag_ref, 1)
    front_loads = [
        load(front_hbm.at[:, :, h], front_out.at[:, h], 2) for h in range(front_out.shape[1])
    ]
    for copy in [map_load, count_load] + near_loads:
        copy.start()

    barrier = pltpu.get_barrier_semaphore()
    for k in range(1, row_count):
        pl.semaphore_signal(
            barrier, inc=1, device_id=((row + k) % row_count, col), device_id_type=MESH
        )
    for other in (x_col, z_col):
        pl.semaphore_signal(barrier, inc=1, device_id=(row, other), device_id_type=MESH)

    def far_copy(k, child, source, par, i, dest_row):
        t, start, size = steps[i]
        part = pl.ds(start, size)
        return remote(
            far_rows.at[k - 1, t, part], rows_out.at[source, 2 * t + par, child, part],
            far_send.at[k - 1], far_recv.at[k - 1, i], dest_row, col,
        )

    def piece_copy(source, par, i, send, recv, to_col):
        t, start, size = steps[i]
        piece = rows_out.at[source, 2 * t + par, :, pl.ds(start, size)]
        return remote(piece, piece, send, recv, row, to_col)

    def far_landed(k, source, par, i):
        return piece_copy(source, par, i, far_send.at[k - 1], far_recv.at[k - 1, i], col)

    def x_copy(k, source, par, i):
        return piece_copy(source, par, i, x_send.at[k - 1], step_recv.at[k - 1, i], x_col)

    def z_copy(k, source, par, i):
        return piece_copy(source, par, i, z_send.at[k - 1], step_recv.at[k - 1, i], z_col)

    def xr_copy(k, source, par, i):
        return piece_copy(source, par, i, relay_send.at[k - 1], relay_recv.at[k - 1], x_col)

    def zr_copy(k, source, par, i):
        return piece_copy(source, par, i, relay_send.at[k - 1], relay_recv.at[k - 1], z_col)

    def all_of(ref, send, recv):
        return remote(ref, ref, send, recv, pair_row, col)

    def pair_copy(child, m):
        return remote(
            pair_rows.at[m], rows_out.at[group, m, child], pair_send, pair_recv, pair_row, col
        )

    def near_copy(child, t):
        piece = cols_out.at[group, t, child]
        return remote(piece, piece, near_send, near_recv, pair_row, col)

    def col_part(source, t, p):
        return cols_out.at[source, t, :, pl.ds(p * rank // 2, rank // 2)]

    def col_copy(k, t, p, dest):
        piece = cols_out.at[group, t, core, pl.ds(p * rank // 2, rank // 2)]
        return remote(
            piece, piece, col_send.at[k - 1], col_recv.at[k - 1, 2 * t + p], 2 * dest + 1, col
        )

    def side_copy(k, source, t, p):
        piece = col_part(source, t, p)
        return remote(piece, piece, side_send.at[k - 1], side_recv.at[k - 1], pair_row, col)

    def swap_copy():
        return remote(
            own_diag.at[pl.ds((1 - core) * part_rows, part_rows)], swap_diag,
            swap_send, swap_recv, pair_row, col,
        )

    def diag_copy():
        return remote(
            sum_diag, diag_in.at[group, pl.ds(core * part_rows, part_rows)],
            diag_send, diag_recv.at[group], diag_row, col,
        )

    map_load.wait()
    count_load.wait()
    gen_load.start()
    coupling_load.start()
    diag_load.start()
    load(near_ref, near_ref, 2).wait()
    for t in range(col_cap):
        for k, dest in far:
            if t == 0:
                found, count = lookup(core, group, far_slot(dest, 0))
                at = jnp.maximum(found - near_start(dest), 0)
                far_rows[k - 1, 0] = masked(near_ref[k - 1, at], count)
            else:
                far_rows[k - 1, t] = masked_rows(far_slot(dest, t))
        if t == 0:
            pl.semaphore_wait(barrier, row_count + 1)
        for i in range(len(steps)):
            if steps[i][0] == t:
                for k, dest in far:
                    far_copy(k, core, group, parity(dest), i, 2 * dest + quarter % 2).start()
        if t == 0:
            gen_load.wait()
    for k, dest in far:
        @pl.when(overlaps(dest))
        def _():
            slot_row = 2 * extra_t + 1 - parity(dest)
            slot = slot_row * row_count + 2 * dest + 1 - quarter % 2
            extra_rows[...] = masked_rows(slot)[extra_start:extra_start + extra_size]
            copy = remote(
                extra_rows, rows_out.at[group, slot_row, core, pl.ds(extra_start, extra_size)],
                extra_send, extra_recv.at[k - 1], 2 * dest + 1 - quarter % 2, col,
            )
            copy.start()

    coupling_load.wait()
    for t in range(col_cap):
        cols_out[group, t, core] = project(core, masked_rows(t * col_count + col))
        near_copy(core, t).start()
        for k, dest in far:
            @pl.when(jnp.logical_not(overlaps(dest)))
            def _():
                for p in range(2):
                    col_copy(k, t, p, dest).start()

    diag_load.wait()
    for copy in front_loads:
        copy.start()
    row_iota2 = lax.broadcasted_iota(jnp.int32, (block, block), 0)
    col_iota2 = lax.broadcasted_iota(jnp.int32, (block, block), 1)
    edge = jnp.maximum(row_iota2, col_iota2)
    for t in range(col_cap):
        found, count = lookup(core, group, t * col_count + col)
        piece = jnp.where(edge < count, diag_ref[found].astype(jnp.float32), 0.0)
        own_diag[t * block:(t + 1) * block, :] = piece.astype(jnp.bfloat16)
    swap_copy().start()

    def send_diag():
        swap_copy().wait_recv()
        own = own_diag[pl.ds(core * part_rows, part_rows), :].astype(jnp.float32)
        total = (own + swap_diag[...].astype(jnp.float32)).astype(jnp.bfloat16)

        @pl.when(row != diag_row)
        def _():
            sum_diag[...] = total
            diag_copy().start()

        @pl.when(row == diag_row)
        def _():
            diag_in[group, pl.ds(core * part_rows, part_rows), :] = total

    def send_pair():
        for m in range(row_cap):
            pair_rows[m] = masked_rows(m * row_count + pair_row)
            pair_copy(core, m).start()

    def keep_own():
        for m in range(row_cap):
            rows_out[group, m, core] = masked_rows(m * row_count + row)

    def add_diag(source):
        for t in range(col_cap):
            b = source * col_cap + t
            total = diag_in[source, t * block:(t + 1) * block, :].astype(jnp.float32)
            spot = pl.ds(b % cols_local, block, stride=cols_local)
            for h in range(block // LANES):
                held = front_out.at[b * ratio + half, h].reshape(block * cols_local, LANES)
                held[spot, :] = held[spot, :] + total[:, h * LANES:(h + 1) * LANES]

    def relay_x(count):
        for i in range(count):
            for k, source in sources:
                z_copy(k, source, 1 - par, i).wait_recv()
                xr_copy(k, source, 1 - par, i).start()

    def relay_z(low, high):
        for i in range(low, high):
            for k, source in sources:
                x_copy(k, source, par, i).wait_recv()
                zr_copy(k, source, par, i).start()

    @pl.when(holder)
    def _():
        for i in range(len(steps)):
            for k, source in sources:
                far_landed(k, source, par, i).wait_recv()
                x_copy(k, source, par, i).start()
                z_copy(k, source, par, i).start()
            if i == 1:
                send_pair()
            if i == middle // 2:
                send_diag()
            if i == middle:
                keep_own()

        @pl.when(overlaps(group))
        def _():
            relay_x(first)

        @pl.when(jnp.logical_not(overlaps(group)))
        def _():
            relay_x(middle)

        @pl.when(overlaps(group))
        def _():
            for k, source in sources:
                for t in range(col_cap):
                    for child in range(2):
                        cols_out[source, t, child] = project(
                            child, rows_out[source, 2 * t + par, child]
                        )
                    for p in range(2):
                        side_copy(k, source, t, p).start()

    @pl.when(jnp.logical_not(holder))
    def _():
        send_pair()
        keep_own()
        send_diag()

        @pl.when(z_over)
        def _():
            relay_z(first, last)

        @pl.when(jnp.logical_not(z_over))
        def _():
            relay_z(middle, len(steps))

    @pl.when(jnp.logical_and(jnp.logical_not(overlaps(group)), core == 1))
    def _():
        for t in range(col_cap):
            for p in range(2):
                for k, source in sources:
                    both = col_part(source, t, p)
                    all_of(both, col_send.at[k - 1], col_recv.at[k - 1, 2 * t + p]).wait_recv()
                    side_copy(k, source, t, p).start()

    load(front_out, front_out, 2).wait()

    @pl.when(row == diag_row)
    def _():
        all_of(sum_diag, diag_send, diag_recv.at[group]).wait_recv()
        add_diag(group)

    all_of(pair_rows, pair_send, pair_recv).wait_recv()
    all_of(pair_rows, pair_send, pair_recv).wait_send()
    all_of(cols_out.at[group, :, 1 - core], near_send, near_recv).wait_recv()
    all_of(cols_out.at[group, :, core], near_send, near_recv).wait_send()
    for k, dest in far:
        all_of(far_rows.at[k - 1], far_send.at[k - 1], relay_recv.at[k - 1]).wait_send()

    swap_copy().wait_send()

    @pl.when(row != diag_row)
    def _():
        diag_copy().wait_send()

    for k, dest in far:
        @pl.when(jnp.logical_not(overlaps(dest)))
        def _():
            all_of(cols_out.at[group, :, core], col_send.at[k - 1], side_recv.at[k - 1]).wait_send()

        @pl.when(overlaps(dest))
        def _():
            all_of(extra_rows, extra_send, extra_recv.at[k - 1]).wait_send()

    @pl.when(row == diag_row)
    def _():
        for k, source in sources:
            all_of(diag_in.at[source], diag_send, diag_recv.at[source]).wait_recv()
            add_diag(source)

    one_part = rows_out.at[group, pl.ds(0, col_cap)]
    half_part = rows_out.at[group, pl.ds(0, col_cap), 0]

    low_part = rows_out.at[group, 0, :, pl.ds(0, part_rows // 2)]
    part_of_extra = rows_out.at[group, 0, :, pl.ds(0, extra_size)]
    over_part = rows_out.at[group, pl.ds(0, 2), :, pl.ds(0, part_rows // 2)]

    @pl.when(holder)
    def _():
        for k, source in sources:
            for i in range(middle, len(steps)):
                z_copy(k, source, 1 - par, i).wait_recv()
            all_of(one_part, x_send.at[k - 1], relay_recv.at[k - 1]).wait_send()
            all_of(one_part, z_send.at[k - 1], relay_recv.at[k - 1]).wait_send()

            @pl.when(overlaps(group))
            def _():
                for i in range(first, middle):
                    z_copy(k, source, 1 - par, i).wait_recv()
                all_of(low_part, relay_send.at[k - 1], relay_recv.at[k - 1]).wait_send()

            @pl.when(jnp.logical_not(overlaps(group)))
            def _():
                all_of(half_part, relay_send.at[k - 1], relay_recv.at[k - 1]).wait_send()

    @pl.when(jnp.logical_not(holder))
    def _():
        for k, source in sources:
            for i in range(first):
                x_copy(k, source, par, i).wait_recv()

            @pl.when(z_over)
            def _():
                for i in range(last, len(steps)):
                    x_copy(k, source, par, i).wait_recv()
                all_of(low_part, relay_send.at[k - 1], relay_recv.at[k - 1]).wait_send()

            @pl.when(jnp.logical_not(z_over))
            def _():
                for i in range(first, middle):
                    x_copy(k, source, par, i).wait_recv()
                all_of(half_part, relay_send.at[k - 1], relay_recv.at[k - 1]).wait_send()

            @pl.when(overlaps(group))
            def _():
                all_of(part_of_extra, extra_send, extra_recv.at[k - 1]).wait_recv()
                all_of(over_part, relay_send.at[k - 1], relay_recv.at[k - 1]).wait_recv()

            @pl.when(jnp.logical_not(overlaps(group)))
            def _():
                all_of(one_part, relay_send.at[k - 1], relay_recv.at[k - 1]).wait_recv()

    gives = jnp.where(overlaps(group), holder, core == 1)
    for k, source in sources:
        side = all_of(cols_out.at[source], side_send.at[k - 1], side_recv.at[k - 1])

        @pl.when(gives)
        def _():
            side.wait_send()

        @pl.when(jnp.logical_not(gives))
        def _():
            side.wait_recv()


def add_kernel(
    front_ref, rows_ref, cols_ref, out_ref, staged, out_sem
):
    rows_local, halves, block, cols_local, _ = front_ref.shape
    _, row_cap, _, _, rank = rows_ref.shape
    col_cap = cols_ref.shape[1]

    for a in range(rows_local):
        s, m = divmod(a, row_cap)
        cuts = (0, block // 2, block) if a < 2 else (0, block)
        for low, high in zip(cuts[:-1], cuts[1:]):
            size = high - low
            rows = jnp.concatenate(
                [rows_ref[s, m, 0, low:high], rows_ref[s, m, 1, low:high]], axis=1
            )
            for b in range(cols_local):
                cols = cols_ref[b // col_cap, b % col_cap].reshape(2 * rank, block)
                tile = jnp.dot(rows, cols, preferred_element_type=jnp.float32)
                spot = pl.ds(low * cols_local + b, size, stride=cols_local)
                for h in range(halves):
                    src = front_ref.at[a, h].reshape(block * cols_local, LANES)
                    dst = staged.at[a, h].reshape(block * cols_local, LANES)
                    dst[spot, :] = src[spot, :] + tile[:, h * LANES:(h + 1) * LANES]
            for h in range(halves):
                pltpu.make_async_copy(
                    staged.at[a, h, low:high], out_ref.at[a, low:high, h], out_sem
                ).start()
    pltpu.make_async_copy(staged, staged, out_sem).wait()


def shards(parent_front, generators, diagonal_blocks, coupling, block_map, valid_rows):
    row_count = lax.axis_size("row")
    col_count = lax.axis_size("col")
    groups = row_count // 2
    block, rank = generators.shape[1:]
    rows_local = parent_front.shape[0]
    cols_local = parent_front.shape[2]
    row_cap = rows_local // groups
    col_cap = cols_local // groups
    vmem = pl.BlockSpec(memory_space=pltpu.VMEM)
    hbm = pl.BlockSpec(memory_space=pltpu.HBM)
    dma = pltpu.SemaphoreType.DMA
    halves = block // LANES
    split = parent_front.reshape(rows_local, block, cols_local, halves, LANES)
    split = split.transpose(0, 1, 3, 2, 4)
    held = (rows_local, halves, block, cols_local, LANES)
    operands = [
        pltpu.with_memory_space_constraint(x, pltpu.HBM)
        for x in (generators, diagonal_blocks, coupling, block_map, valid_rows, split)
    ]
    far = groups - 1
    group_blocks = generators.shape[0]
    near = (far, row_cap * row_count - group_blocks + 1, block, rank)
    extra = (col_cap * block // 2, rank)
    rows, cols, front = pl.pallas_call(
        functools.partial(exchange_kernel, row_count, col_count, row_cap, col_cap),
        out_shape=(
            pltpu.VMEM((groups, row_cap, 2, block, rank), jnp.bfloat16),
            pltpu.VMEM((groups, col_cap, 2, rank, block), jnp.bfloat16),
            pltpu.VMEM(held, jnp.float32),
        ),
        in_specs=[hbm] * 6,
        out_specs=(vmem,) * 3,
        scratch_shapes=[
            pltpu.VMEM(generators.shape, jnp.bfloat16),
            pltpu.VMEM(near, jnp.bfloat16),
            pltpu.VMEM(diagonal_blocks.shape, jnp.bfloat16),
            pltpu.VMEM(coupling.shape, jnp.bfloat16),
            pltpu.SMEM(block_map.shape, jnp.int32),
            pltpu.SMEM(valid_rows.shape, jnp.int32),
            dma((4,)),
            pltpu.VMEM((far, col_cap, block, rank), jnp.bfloat16),
            pltpu.VMEM(extra, jnp.bfloat16),
            pltpu.VMEM((row_cap, block, rank), jnp.bfloat16),
            pltpu.VMEM((col_cap * block, block), jnp.bfloat16),
            pltpu.VMEM((col_cap * block // 2, block), jnp.bfloat16),
            pltpu.VMEM((col_cap * block // 2, block), jnp.bfloat16),
            pltpu.VMEM((groups, col_cap * block, block), jnp.bfloat16),
            dma((far,)),
            dma((far, STEPS)),
            dma((far,)),
            dma((far,)),
            dma((far, STEPS)),
            dma((far,)),
            dma((far,)),
            dma,
            dma,
            dma,
            dma,
            dma((far,)),
            dma((far, 2 * col_cap)),
            dma((far,)),
            dma((far,)),
            dma,
            dma,
            dma,
            dma((groups,)),
            dma,
            dma((far,)),
        ],
        compiler_params=pltpu.CompilerParams(
            collective_id=0, has_side_effects=True, vmem_limit_bytes=32 * 1024 * 1024
        ),
    )(*operands)
    out = pl.pallas_call(
        add_kernel,
        out_shape=jax.ShapeDtypeStruct(split.shape, jnp.float32),
        in_specs=[vmem] * 3,
        out_specs=hbm,
        scratch_shapes=[pltpu.VMEM(held, jnp.float32), dma],
        compiler_params=pltpu.CompilerParams(vmem_limit_bytes=32 * 1024 * 1024),
    )(*(pltpu.with_memory_space_constraint(x, pltpu.VMEM) for x in (front, rows, cols)))
    return out.transpose(0, 1, 3, 2, 4).reshape(parent_front.shape)


def solution(mesh):
    in_specs = (
        P(None, "row", None, "col"),
        P("row", None, None),
        P("row", None, None),
        P(),
        P(),
        P(),
    )
    out_specs = P(None, "row", None, "col")
    return jax.shard_map(shards, mesh=mesh, in_specs=in_specs, out_specs=out_specs, check_vma=False)
```

```python
import functools

import jax
import jax.numpy as jnp
from jax import lax
from jax.experimental import pallas as pl
from jax.experimental.pallas import tpu as pltpu
from jax.sharding import PartitionSpec as P

MESH = pl.DeviceIdType.MESH
QUAD = 4
STEPS = 16
LANES = 128


def steps_of(col_cap, block):
    per_block = STEPS // col_cap
    size = block // per_block
    return [(t, p * size, size) for t in range(col_cap) for p in range(per_block)]


def exchange_kernel(
    row_count, col_count, row_cap, col_cap,
    gen_hbm, diag_hbm, coupling_hbm, map_hbm, count_hbm, front_hbm,
    rows_out, cols_out, front_out,
    gen_ref, near_ref, diag_ref, coupling_ref, map_ref, count_ref, load_sem,
    far_rows, extra_rows, pair_rows, own_diag, swap_diag, sum_diag, diag_in,
    far_send, far_recv, both_send, z_recv, relay_send, relay_recv,
    pair_send, pair_recv, near_send, near_recv, col_send, col_recv, side_send, side_recv,
    swap_send, swap_recv, diag_send, diag_recv, extra_send, extra_recv,
):
    groups = row_count // 2
    group_blocks, block, rank = gen_ref.shape
    window = row_cap * row_count
    steps = steps_of(col_cap, block)
    middle = len(steps) // 2
    first = middle - 2
    last = middle + 1
    step_rows = steps[0][2]
    part_rows = col_cap * block // 2
    extra_size = (len(steps) - last) * step_rows
    extra_t, extra_start, _ = steps[last]
    ratio = col_count // row_count
    cols_local = groups * col_cap
    row = lax.axis_index("row")
    col = lax.axis_index("col")
    group = row // 2
    core = row % 2
    quarter = col % QUAD
    half = col // row_count
    pair_row = group * 2 + 1 - core
    diag_row = col % row_count
    x_col = col + 1 - 2 * (quarter % 2)
    z_col = col + 2 - 4 * (quarter // 2)
    holder = quarter % 2 == core

    def parity(dest):
        return jnp.where(quarter // 2 == dest % 2, half, 1 - half)

    def overlaps(dest):
        return diag_row // 2 == dest

    z_over = (z_col % row_count) // 2 == group

    def lookup(child, source, slot):
        found = jnp.int32(0)
        count = jnp.int32(0)
        target = source * window + slot
        for d in range(window - group_blocks + 1):
            k = jnp.clip(slot - d, 0, group_blocks - 1)
            hit = map_ref[child, source * group_blocks + k] == target
            found = jnp.where(hit, k, found)
            count = jnp.where(hit, count_ref[child, source * group_blocks + k], count)
        return found, count

    row_iota = lax.broadcasted_iota(jnp.int32, (block, LANES), 0)

    def masked(rows, count):
        kept = (row_iota < count).astype(jnp.float32).astype(jnp.bfloat16)
        return rows * jnp.concatenate([kept] * (rank // LANES), axis=1)

    def masked_rows(slot):
        found, count = lookup(core, group, slot)
        return masked(gen_ref[found], count)

    def project(child, rows):
        return lax.dot_general(
            coupling_ref[child], rows, (((0,), (1,)), ((), ())),
            preferred_element_type=jnp.float32,
        ).astype(jnp.bfloat16)

    def remote(src, dst, send, recv, to_row, to_col):
        return pltpu.make_async_remote_copy(
            src_ref=src, dst_ref=dst, send_sem=send, recv_sem=recv,
            device_id=(to_row, to_col), device_id_type=MESH,
        )

    def load(src, dst, n):
        return pltpu.make_async_copy(src, dst, load_sem.at[n])

    far = [(k, (group + k) % groups) for k in range(1, groups)]
    sources = [(k, (group + groups - k) % groups) for k in range(1, groups)]
    par = parity(group)
    spread = near_ref.shape[1]

    def far_slot(dest, t):
        return (2 * t + parity(dest)) * row_count + 2 * dest + quarter % 2

    def near_start(dest):
        return jnp.clip(far_slot(dest, 0) - spread + 1, 0, group_blocks - spread)

    map_load = load(map_hbm, map_ref, 0)
    count_load = load(count_hbm, count_ref, 1)
    near_loads = [
        load(gen_hbm.at[pl.ds(near_start(dest), spread)], near_ref.at[k - 1], 2) for k, dest in far
    ]
    gen_load = load(gen_hbm, gen_ref, 3)
    coupling_load = load(coupling_hbm, coupling_ref, 0)
    diag_load = load(diag_hbm, diag_ref, 1)
    front_loads = [
        load(front_hbm.at[:, :, h], front_out.at[:, h], 2) for h in range(front_out.shape[1])
    ]
    for copy in [map_load, count_load] + near_loads:
        copy.start()

    barrier = pltpu.get_barrier_semaphore()
    for k in range(1, row_count):
        pl.semaphore_signal(
            barrier, inc=1, device_id=((row + k) % row_count, col), device_id_type=MESH
        )
    for other in (x_col, z_col):
        pl.semaphore_signal(barrier, inc=1, device_id=(row, other), device_id_type=MESH)

    def far_copy(k, child, source, par, i, dest_row):
        t, start, size = steps[i]
        part = pl.ds(start, size)
        return remote(
            far_rows.at[k - 1, t, part], rows_out.at[source, 2 * t + par, child, part],
            far_send.at[k - 1], far_recv.at[k - 1, i], dest_row, col,
        )

    def piece_copy(source, par, i, send, recv, to_col):
        t, start, size = steps[i]
        piece = rows_out.at[source, 2 * t + par, :, pl.ds(start, size)]
        return remote(piece, piece, send, recv, row, to_col)

    def far_landed(k, source, par, i):
        return piece_copy(source, par, i, far_send.at[k - 1], far_recv.at[k - 1, i], col)

    def x_copy(k, source, par, i):
        return piece_copy(source, par, i, both_send.at[k - 1], far_recv.at[k - 1, i], x_col)

    def z_copy(k, source, par, i):
        return piece_copy(source, par, i, both_send.at[k - 1], z_recv.at[k - 1, min(i, middle)], z_col)

    def xr_copy(k, source, par, i):
        return piece_copy(source, par, i, relay_send.at[k - 1], relay_recv.at[k - 1, 0], x_col)

    def zr_copy(k, source, par, i):
        return piece_copy(source, par, i, relay_send.at[k - 1], relay_recv.at[k - 1, 1], z_col)

    def all_of(ref, send, recv):
        return remote(ref, ref, send, recv, pair_row, col)

    def pair_copy(child, m):
        return remote(
            pair_rows.at[m], rows_out.at[group, m, child], pair_send, pair_recv, pair_row, col
        )

    def near_copy(child, t):
        piece = cols_out.at[group, t, child]
        return remote(piece, piece, near_send, near_recv, pair_row, col)

    def col_part(source, t, p):
        return cols_out.at[source, t, :, pl.ds(p * rank // 2, rank // 2)]

    def col_copy(k, t, p, dest):
        piece = cols_out.at[group, t, core, pl.ds(p * rank // 2, rank // 2)]
        return remote(
            piece, piece, col_send.at[k - 1], col_recv.at[k - 1, 2 * t + p], 2 * dest + 1, col
        )

    def side_copy(k, source, t, p):
        piece = col_part(source, t, p)
        return remote(piece, piece, side_send.at[k - 1], side_recv.at[k - 1], pair_row, col)

    def swap_copy():
        return remote(
            own_diag.at[pl.ds((1 - core) * part_rows, part_rows)], swap_diag,
            swap_send, swap_recv, pair_row, col,
        )

    def diag_copy():
        return remote(
            sum_diag, diag_in.at[group, pl.ds(core * part_rows, part_rows)],
            diag_send, diag_recv.at[group], diag_row, col,
        )

    map_load.wait()
    count_load.wait()
    gen_load.start()
    coupling_load.start()
    diag_load.start()
    load(near_ref, near_ref, 2).wait()
    for t in range(col_cap):
        for k, dest in far:
            if t == 0:
                found, count = lookup(core, group, far_slot(dest, 0))
                at = jnp.maximum(found - near_start(dest), 0)
                far_rows[k - 1, 0] = masked(near_ref[k - 1, at], count)
            else:
                far_rows[k - 1, t] = masked_rows(far_slot(dest, t))
        if t == 0:
            pl.semaphore_wait(barrier, row_count + 1)
        for i in range(len(steps)):
            if steps[i][0] == t:
                for k, dest in far:
                    far_copy(k, core, group, parity(dest), i, 2 * dest + quarter % 2).start()
        if t == 0:
            gen_load.wait()
    for k, dest in far:
        @pl.when(overlaps(dest))
        def _():
            slot_row = 2 * extra_t + 1 - parity(dest)
            slot = slot_row * row_count + 2 * dest + 1 - quarter % 2
            extra_rows[...] = masked_rows(slot)[extra_start:extra_start + extra_size]
            copy = remote(
                extra_rows, rows_out.at[group, slot_row, core, pl.ds(extra_start, extra_size)],
                extra_send, extra_recv.at[k - 1], 2 * dest + 1 - quarter % 2, col,
            )
            copy.start()

    coupling_load.wait()
    for t in range(col_cap):
        cols_out[group, t, core] = project(core, masked_rows(t * col_count + col))
        near_copy(core, t).start()
        for k, dest in far:
            @pl.when(jnp.logical_not(overlaps(dest)))
            def _():
                for p in range(2):
                    col_copy(k, t, p, dest).start()

    diag_load.wait()
    for copy in front_loads:
        copy.start()
    row_iota2 = lax.broadcasted_iota(jnp.int32, (block, block), 0)
    col_iota2 = lax.broadcasted_iota(jnp.int32, (block, block), 1)
    edge = jnp.maximum(row_iota2, col_iota2)
    for t in range(col_cap):
        found, count = lookup(core, group, t * col_count + col)
        piece = jnp.where(edge < count, diag_ref[found].astype(jnp.float32), 0.0)
        own_diag[t * block:(t + 1) * block, :] = piece.astype(jnp.bfloat16)
    swap_copy().start()

    def send_diag():
        swap_copy().wait_recv()
        own = own_diag[pl.ds(core * part_rows, part_rows), :].astype(jnp.float32)
        total = (own + swap_diag[...].astype(jnp.float32)).astype(jnp.bfloat16)

        @pl.when(row != diag_row)
        def _():
            sum_diag[...] = total
            diag_copy().start()

        @pl.when(row == diag_row)
        def _():
            diag_in[group, pl.ds(core * part_rows, part_rows), :] = total

    def send_pair():
        for m in range(row_cap):
            pair_rows[m] = masked_rows(m * row_count + pair_row)
            pair_copy(core, m).start()

    def keep_own():
        for m in range(row_cap):
            rows_out[group, m, core] = masked_rows(m * row_count + row)

    def add_diag(source):
        for t in range(col_cap):
            b = source * col_cap + t
            total = diag_in[source, t * block:(t + 1) * block, :].astype(jnp.float32)
            spot = pl.ds(b % cols_local, block, stride=cols_local)
            for h in range(block // LANES):
                held = front_out.at[b * ratio + half, h].reshape(block * cols_local, LANES)
                held[spot, :] = held[spot, :] + total[:, h * LANES:(h + 1) * LANES]

    def relay_x(count):
        for i in range(count):
            for k, source in sources:
                z_copy(k, source, 1 - par, i).wait_recv()
                xr_copy(k, source, 1 - par, i).start()

    def relay_z(low, high):
        for i in range(low, high):
            for k, source in sources:
                x_copy(k, source, par, i).wait_recv()
                zr_copy(k, source, par, i).start()

    @pl.when(holder)
    def _():
        for i in range(len(steps)):
            for k, source in sources:
                far_landed(k, source, par, i).wait_recv()
                x_copy(k, source, par, i).start()
                z_copy(k, source, par, i).start()
            if i == 1:
                send_pair()
            if i == middle // 2:
                send_diag()
            if i == middle:
                keep_own()

        @pl.when(overlaps(group))
        def _():
            relay_x(first)

        @pl.when(jnp.logical_not(overlaps(group)))
        def _():
            relay_x(middle)

        @pl.when(overlaps(group))
        def _():
            for k, source in sources:
                for t in range(col_cap):
                    for child in range(2):
                        cols_out[source, t, child] = project(
                            child, rows_out[source, 2 * t + par, child]
                        )
                    for p in range(2):
                        side_copy(k, source, t, p).start()

    @pl.when(jnp.logical_not(holder))
    def _():
        send_pair()
        keep_own()
        send_diag()

        @pl.when(z_over)
        def _():
            relay_z(first, last)

        @pl.when(jnp.logical_not(z_over))
        def _():
            relay_z(middle, len(steps))

    @pl.when(jnp.logical_and(jnp.logical_not(overlaps(group)), core == 1))
    def _():
        for t in range(col_cap):
            for p in range(2):
                for k, source in sources:
                    both = col_part(source, t, p)
                    all_of(both, col_send.at[k - 1], col_recv.at[k - 1, 2 * t + p]).wait_recv()
                    side_copy(k, source, t, p).start()

    load(front_out, front_out, 2).wait()

    @pl.when(row == diag_row)
    def _():
        all_of(sum_diag, diag_send, diag_recv.at[group]).wait_recv()
        add_diag(group)

    all_of(pair_rows, pair_send, pair_recv).wait_recv()
    all_of(pair_rows, pair_send, pair_recv).wait_send()
    all_of(cols_out.at[group, :, 1 - core], near_send, near_recv).wait_recv()
    all_of(cols_out.at[group, :, core], near_send, near_recv).wait_send()
    for k, dest in far:
        all_of(far_rows.at[k - 1], far_send.at[k - 1], relay_recv.at[k - 1, 0]).wait_send()

    swap_copy().wait_send()

    @pl.when(row != diag_row)
    def _():
        diag_copy().wait_send()

    for k, dest in far:
        @pl.when(jnp.logical_not(overlaps(dest)))
        def _():
            all_of(cols_out.at[group, :, core], col_send.at[k - 1], side_recv.at[k - 1]).wait_send()

        @pl.when(overlaps(dest))
        def _():
            all_of(extra_rows, extra_send, extra_recv.at[k - 1]).wait_send()

    @pl.when(row == diag_row)
    def _():
        for k, source in sources:
            all_of(diag_in.at[source], diag_send, diag_recv.at[source]).wait_recv()
            add_diag(source)

    def rows_of(count):
        return rows_out.at[group, 0, :, pl.ds(0, count * step_rows)]

    def relayed(k, count, way):
        return all_of(rows_of(count), relay_send.at[k - 1], relay_recv.at[k - 1, way])

    rest = len(steps) - middle

    @pl.when(holder)
    def _():
        for k, source in sources:
            all_of(rows_of(rest), both_send.at[k - 1], z_recv.at[k - 1, middle]).wait_recv()
            all_of(rows_out.at[group], both_send.at[k - 1], z_recv.at[k - 1, 0]).wait_send()

            @pl.when(overlaps(group))
            def _():
                for i in range(first, middle):
                    z_copy(k, source, 1 - par, i).wait_recv()
                relayed(k, first, 0).wait_send()

            @pl.when(jnp.logical_not(overlaps(group)))
            def _():
                relayed(k, middle, 0).wait_send()

    @pl.when(jnp.logical_not(holder))
    def _():
        for k, source in sources:
            for i in range(first):
                x_copy(k, source, par, i).wait_recv()

            @pl.when(z_over)
            def _():
                for i in range(last, len(steps)):
                    x_copy(k, source, par, i).wait_recv()
                relayed(k, last - first, 0).wait_send()

            @pl.when(jnp.logical_not(z_over))
            def _():
                for i in range(first, middle):
                    x_copy(k, source, par, i).wait_recv()
                relayed(k, rest, 0).wait_send()

            @pl.when(overlaps(group))
            def _():
                all_of(rows_of(len(steps) - last), extra_send, extra_recv.at[k - 1]).wait_recv()
                relayed(k, first, 0).wait_recv()
                relayed(k, last - first, 1).wait_recv()

            @pl.when(jnp.logical_not(overlaps(group)))
            def _():
                relayed(k, middle, 0).wait_recv()
                relayed(k, rest, 1).wait_recv()

    gives = jnp.where(overlaps(group), holder, core == 1)
    for k, source in sources:
        side = all_of(cols_out.at[source], side_send.at[k - 1], side_recv.at[k - 1])

        @pl.when(gives)
        def _():
            side.wait_send()

        @pl.when(jnp.logical_not(gives))
        def _():
            side.wait_recv()


def add_kernel(
    front_ref, rows_ref, cols_ref, out_ref, staged, out_sem
):
    rows_local, halves, block, cols_local, _ = front_ref.shape
    _, row_cap, _, _, rank = rows_ref.shape
    col_cap = cols_ref.shape[1]

    for a in range(rows_local):
        s, m = divmod(a, row_cap)
        cuts = (0, block // 2, block) if a < 2 else (0, block)
        for low, high in zip(cuts[:-1], cuts[1:]):
            size = high - low
            rows = jnp.concatenate(
                [rows_ref[s, m, 0, low:high], rows_ref[s, m, 1, low:high]], axis=1
            )
            for b in range(cols_local):
                cols = cols_ref[b // col_cap, b % col_cap].reshape(2 * rank, block)
                tile = jnp.dot(rows, cols, preferred_element_type=jnp.float32)
                spot = pl.ds(low * cols_local + b, size, stride=cols_local)
                for h in range(halves):
                    src = front_ref.at[a, h].reshape(block * cols_local, LANES)
                    dst = staged.at[a, h].reshape(block * cols_local, LANES)
                    dst[spot, :] = src[spot, :] + tile[:, h * LANES:(h + 1) * LANES]
            for h in range(halves):
                pltpu.make_async_copy(
                    staged.at[a, h, low:high], out_ref.at[a, low:high, h], out_sem
                ).start()
    pltpu.make_async_copy(staged, staged, out_sem).wait()


def shards(parent_front, generators, diagonal_blocks, coupling, block_map, valid_rows):
    row_count = lax.axis_size("row")
    col_count = lax.axis_size("col")
    groups = row_count // 2
    block, rank = generators.shape[1:]
    rows_local = parent_front.shape[0]
    cols_local = parent_front.shape[2]
    row_cap = rows_local // groups
    col_cap = cols_local // groups
    vmem = pl.BlockSpec(memory_space=pltpu.VMEM)
    hbm = pl.BlockSpec(memory_space=pltpu.HBM)
    dma = pltpu.SemaphoreType.DMA
    halves = block // LANES
    split = parent_front.reshape(rows_local, block, cols_local, halves, LANES)
    split = split.transpose(0, 1, 3, 2, 4)
    held = (rows_local, halves, block, cols_local, LANES)
    operands = [
        pltpu.with_memory_space_constraint(x, pltpu.HBM)
        for x in (generators, diagonal_blocks, coupling, block_map, valid_rows, split)
    ]
    far = groups - 1
    group_blocks = generators.shape[0]
    near = (far, row_cap * row_count - group_blocks + 1, block, rank)
    extra = (col_cap * block * (STEPS // 2 - 1) // STEPS, rank)
    rows, cols, front = pl.pallas_call(
        functools.partial(exchange_kernel, row_count, col_count, row_cap, col_cap),
        out_shape=(
            pltpu.VMEM((groups, row_cap, 2, block, rank), jnp.bfloat16),
            pltpu.VMEM((groups, col_cap, 2, rank, block), jnp.bfloat16),
            pltpu.VMEM(held, jnp.float32),
        ),
        in_specs=[hbm] * 6,
        out_specs=(vmem,) * 3,
        scratch_shapes=[
            pltpu.VMEM(generators.shape, jnp.bfloat16),
            pltpu.VMEM(near, jnp.bfloat16),
            pltpu.VMEM(diagonal_blocks.shape, jnp.bfloat16),
            pltpu.VMEM(coupling.shape, jnp.bfloat16),
            pltpu.SMEM(block_map.shape, jnp.int32),
            pltpu.SMEM(valid_rows.shape, jnp.int32),
            dma((4,)),
            pltpu.VMEM((far, col_cap, block, rank), jnp.bfloat16),
            pltpu.VMEM(extra, jnp.bfloat16),
            pltpu.VMEM((row_cap, block, rank), jnp.bfloat16),
            pltpu.VMEM((col_cap * block, block), jnp.bfloat16),
            pltpu.VMEM((col_cap * block // 2, block), jnp.bfloat16),
            pltpu.VMEM((col_cap * block // 2, block), jnp.bfloat16),
            pltpu.VMEM((groups, col_cap * block, block), jnp.bfloat16),
            dma((far,)),
            dma((far, STEPS)),
            dma((far,)),
            dma((far, STEPS // 2 + 1)),
            dma((far,)),
            dma((far, 2)),
            dma,
            dma,
            dma,
            dma,
            dma((far,)),
            dma((far, 2 * col_cap)),
            dma((far,)),
            dma((far,)),
            dma,
            dma,
            dma,
            dma((groups,)),
            dma,
            dma((far,)),
        ],
        compiler_params=pltpu.CompilerParams(
            collective_id=0, has_side_effects=True, vmem_limit_bytes=32 * 1024 * 1024
        ),
    )(*operands)
    out = pl.pallas_call(
        add_kernel,
        out_shape=jax.ShapeDtypeStruct(split.shape, jnp.float32),
        in_specs=[vmem] * 3,
        out_specs=hbm,
        scratch_shapes=[pltpu.VMEM(held, jnp.float32), dma],
        compiler_params=pltpu.CompilerParams(vmem_limit_bytes=32 * 1024 * 1024),
    )(*(pltpu.with_memory_space_constraint(x, pltpu.VMEM) for x in (front, rows, cols)))
    return out.transpose(0, 1, 3, 2, 4).reshape(parent_front.shape)


def solution(mesh):
    in_specs = (
        P(None, "row", None, "col"),
        P("row", None, None),
        P("row", None, None),
        P(),
        P(),
        P(),
    )
    out_specs = P(None, "row", None, "col")
    return jax.shard_map(shards, mesh=mesh, in_specs=in_specs, out_specs=out_specs, check_vma=False)
```

```python
import functools

import jax
import jax.numpy as jnp
from jax import lax
from jax.experimental import pallas as pl
from jax.experimental.pallas import tpu as pltpu
from jax.sharding import PartitionSpec as P

MESH = pl.DeviceIdType.MESH
QUAD = 4
UNITS = 16
SIZES = (1, 1, 1, 1, 1, 1, 1, 1, 1, 1, 1, 1, 1, 1, 1, 1)
HALF_AT = 8
FIRST_AT = 6
LAST_AT = 9
LANES = 128


def steps_of(col_cap, block):
    unit = col_cap * block // UNITS
    steps = []
    start = 0
    for size in SIZES:
        steps.append((start // block, start % block, size * unit))
        start += size * unit
    return steps


def exchange_kernel(
    row_count, col_count, row_cap, col_cap,
    gen_hbm, diag_hbm, coupling_hbm, map_hbm, count_hbm, front_hbm,
    rows_out, cols_out, front_out,
    gen_ref, near_ref, diag_ref, coupling_ref, map_ref, count_ref, load_sem,
    far_rows, extra_rows, pair_rows, own_diag, swap_diag, sum_diag, diag_in,
    far_send, far_recv, both_send, z_recv, relay_send, relay_recv,
    pair_send, pair_recv, near_send, near_recv, col_send, col_recv, side_send, side_recv,
    swap_send, swap_recv, diag_send, diag_recv, extra_send, extra_recv,
):
    groups = row_count // 2
    group_blocks, block, rank = gen_ref.shape
    window = row_cap * row_count
    steps = steps_of(col_cap, block)
    middle = HALF_AT
    first = FIRST_AT
    last = LAST_AT
    part_rows = col_cap * block // 2
    extra_size = sum(size for _, _, size in steps[last:])
    extra_t, extra_start, _ = steps[last]
    ratio = col_count // row_count
    cols_local = groups * col_cap
    row = lax.axis_index("row")
    col = lax.axis_index("col")
    group = row // 2
    core = row % 2
    quarter = col % QUAD
    half = col // row_count
    pair_row = group * 2 + 1 - core
    diag_row = col % row_count
    x_col = col + 1 - 2 * (quarter % 2)
    z_col = col + 2 - 4 * (quarter // 2)
    holder = quarter % 2 == core

    def parity(dest):
        return jnp.where(quarter // 2 == dest % 2, half, 1 - half)

    def overlaps(dest):
        return diag_row // 2 == dest

    z_over = (z_col % row_count) // 2 == group

    def lookup(child, source, slot):
        found = jnp.int32(0)
        count = jnp.int32(0)
        target = source * window + slot
        for d in range(window - group_blocks + 1):
            k = jnp.clip(slot - d, 0, group_blocks - 1)
            hit = map_ref[child, source * group_blocks + k] == target
            found = jnp.where(hit, k, found)
            count = jnp.where(hit, count_ref[child, source * group_blocks + k], count)
        return found, count

    row_iota = lax.broadcasted_iota(jnp.int32, (block, LANES), 0)

    def masked(rows, count):
        kept = (row_iota < count).astype(jnp.float32).astype(jnp.bfloat16)
        return rows * jnp.concatenate([kept] * (rank // LANES), axis=1)

    def masked_rows(slot):
        found, count = lookup(core, group, slot)
        return masked(gen_ref[found], count)

    def project(child, rows):
        return lax.dot_general(
            coupling_ref[child], rows, (((0,), (1,)), ((), ())),
            preferred_element_type=jnp.float32,
        ).astype(jnp.bfloat16)

    def remote(src, dst, send, recv, to_row, to_col):
        return pltpu.make_async_remote_copy(
            src_ref=src, dst_ref=dst, send_sem=send, recv_sem=recv,
            device_id=(to_row, to_col), device_id_type=MESH,
        )

    def load(src, dst, n):
        return pltpu.make_async_copy(src, dst, load_sem.at[n])

    barrier = pltpu.get_barrier_semaphore()
    for k in range(1, row_count):
        pl.semaphore_signal(
            barrier, inc=1, device_id=((row + k) % row_count, col), device_id_type=MESH
        )
    for other in (x_col, z_col):
        pl.semaphore_signal(barrier, inc=1, device_id=(row, other), device_id_type=MESH)

    far = [(k, (group + k) % groups) for k in range(1, groups)]
    sources = [(k, (group + groups - k) % groups) for k in range(1, groups)]
    par = parity(group)
    spread = near_ref.shape[1]

    def far_slot(dest, t):
        return (2 * t + parity(dest)) * row_count + 2 * dest + quarter % 2

    def near_start(dest):
        return jnp.clip(far_slot(dest, 0) - spread + 1, 0, group_blocks - spread)

    map_load = load(map_hbm, map_ref, 0)
    count_load = load(count_hbm, count_ref, 1)
    near_loads = [
        load(gen_hbm.at[pl.ds(near_start(dest), spread)], near_ref.at[k - 1], 2) for k, dest in far
    ]
    gen_load = load(gen_hbm, gen_ref, 3)
    coupling_load = load(coupling_hbm, coupling_ref, 0)
    diag_load = load(diag_hbm, diag_ref, 1)
    front_loads = [
        load(front_hbm.at[:, :, h], front_out.at[:, h], 2) for h in range(front_out.shape[1])
    ]
    for copy in [map_load, count_load] + near_loads:
        copy.start()

    def far_copy(k, child, source, par, i, dest_row):
        t, start, size = steps[i]
        part = pl.ds(start, size)
        return remote(
            far_rows.at[k - 1, t, part], rows_out.at[source, 2 * t + par, child, part],
            far_send.at[k - 1], far_recv.at[k - 1, i], dest_row, col,
        )

    def piece_copy(source, par, i, send, recv, to_col):
        t, start, size = steps[i]
        piece = rows_out.at[source, 2 * t + par, :, pl.ds(start, size)]
        return remote(piece, piece, send, recv, row, to_col)

    def far_landed(k, source, par, i):
        return piece_copy(source, par, i, far_send.at[k - 1], far_recv.at[k - 1, i], col)

    def x_copy(k, source, par, i):
        return piece_copy(source, par, i, both_send.at[k - 1], far_recv.at[k - 1, i], x_col)

    def z_copy(k, source, par, i):
        return piece_copy(source, par, i, both_send.at[k - 1], z_recv.at[k - 1, min(i, middle)], z_col)

    def xr_copy(k, source, par, i):
        return piece_copy(source, par, i, relay_send.at[k - 1], relay_recv.at[k - 1, 0], x_col)

    def zr_copy(k, source, par, i):
        return piece_copy(source, par, i, relay_send.at[k - 1], relay_recv.at[k - 1, 1], z_col)

    def all_of(ref, send, recv):
        return remote(ref, ref, send, recv, pair_row, col)

    def pair_copy(child, m):
        return remote(
            pair_rows.at[m], rows_out.at[group, m, child], pair_send, pair_recv, pair_row, col
        )

    def near_copy(child, t):
        piece = cols_out.at[group, t, child]
        return remote(piece, piece, near_send, near_recv, pair_row, col)

    def col_part(source, t, p):
        return cols_out.at[source, t, :, pl.ds(p * rank * 3 // 4, rank * (3 - 2 * p) // 4)]

    def col_copy(k, t, p, dest):
        piece = cols_out.at[group, t, core, pl.ds(p * rank * 3 // 4, rank * (3 - 2 * p) // 4)]
        return remote(
            piece, piece, col_send.at[k - 1], col_recv.at[k - 1, 2 * t + p], 2 * dest + 1, col
        )

    def side_copy(k, source, t, p):
        piece = col_part(source, t, p)
        return remote(piece, piece, side_send.at[k - 1], side_recv.at[k - 1], pair_row, col)

    def swap_copy():
        return remote(
            own_diag.at[pl.ds((1 - core) * part_rows, part_rows)], swap_diag,
            swap_send, swap_recv, pair_row, col,
        )

    def diag_copy():
        return remote(
            sum_diag, diag_in.at[group, pl.ds(core * part_rows, part_rows)],
            diag_send, diag_recv.at[group], diag_row, col,
        )

    map_load.wait()
    count_load.wait()
    gen_load.start()
    coupling_load.start()
    diag_load.start()
    load(near_ref, near_ref, 2).wait()
    for t in range(col_cap):
        for k, dest in far:
            if t == 0:
                found, count = lookup(core, group, far_slot(dest, 0))
                at = jnp.maximum(found - near_start(dest), 0)
                far_rows[k - 1, 0] = masked(near_ref[k - 1, at], count)
            else:
                far_rows[k - 1, t] = masked_rows(far_slot(dest, t))
        if t == 0:
            pl.semaphore_wait(barrier, row_count + 1)
        for i in range(len(steps)):
            if steps[i][0] == t:
                for k, dest in far:
                    far_copy(k, core, group, parity(dest), i, 2 * dest + quarter % 2).start()
        if t == 0:
            gen_load.wait()
    for k, dest in far:
        @pl.when(overlaps(dest))
        def _():
            slot_row = 2 * extra_t + 1 - parity(dest)
            slot = slot_row * row_count + 2 * dest + 1 - quarter % 2
            extra_rows[...] = masked_rows(slot)[extra_start:extra_start + extra_size]
            copy = remote(
                extra_rows, rows_out.at[group, slot_row, core, pl.ds(extra_start, extra_size)],
                extra_send, extra_recv.at[k - 1], 2 * dest + 1 - quarter % 2, col,
            )
            copy.start()

    coupling_load.wait()
    for t in range(col_cap):
        cols_out[group, t, core] = project(core, masked_rows(t * col_count + col))
        near_copy(core, t).start()
        for k, dest in far:
            @pl.when(jnp.logical_not(overlaps(dest)))
            def _():
                for p in range(2):
                    col_copy(k, t, p, dest).start()

    diag_load.wait()
    for copy in front_loads:
        copy.start()
    row_iota2 = lax.broadcasted_iota(jnp.int32, (block, block), 0)
    col_iota2 = lax.broadcasted_iota(jnp.int32, (block, block), 1)
    edge = jnp.maximum(row_iota2, col_iota2)
    for t in range(col_cap):
        found, count = lookup(core, group, t * col_count + col)
        piece = jnp.where(edge < count, diag_ref[found].astype(jnp.float32), 0.0)
        own_diag[t * block:(t + 1) * block, :] = piece.astype(jnp.bfloat16)
    swap_copy().start()

    def send_diag():
        swap_copy().wait_recv()
        own = own_diag[pl.ds(core * part_rows, part_rows), :].astype(jnp.float32)
        total = (own + swap_diag[...].astype(jnp.float32)).astype(jnp.bfloat16)

        @pl.when(row != diag_row)
        def _():
            sum_diag[...] = total
            diag_copy().start()

        @pl.when(row == diag_row)
        def _():
            diag_in[group, pl.ds(core * part_rows, part_rows), :] = total

    def send_pair():
        for m in range(row_cap):
            pair_rows[m] = masked_rows(m * row_count + pair_row)
            pair_copy(core, m).start()

    def keep_own():
        for m in range(row_cap):
            rows_out[group, m, core] = masked_rows(m * row_count + row)

    def add_diag(source):
        for t in range(col_cap):
            b = source * col_cap + t
            total = diag_in[source, t * block:(t + 1) * block, :].astype(jnp.float32)
            spot = pl.ds(b % cols_local, block, stride=cols_local)
            for h in range(block // LANES):
                held = front_out.at[b * ratio + half, h].reshape(block * cols_local, LANES)
                held[spot, :] = held[spot, :] + total[:, h * LANES:(h + 1) * LANES]

    def relay_x(count):
        for i in range(count):
            for k, source in sources:
                z_copy(k, source, 1 - par, i).wait_recv()
                xr_copy(k, source, 1 - par, i).start()

    def relay_z(low, high):
        for i in range(low, high):
            for k, source in sources:
                x_copy(k, source, par, i).wait_recv()
                zr_copy(k, source, par, i).start()

    @pl.when(holder)
    def _():
        for i in range(len(steps)):
            for k, source in sources:
                far_landed(k, source, par, i).wait_recv()
                x_copy(k, source, par, i).start()
                z_copy(k, source, par, i).start()
            if i == 1:
                send_pair()
            if i == middle // 2:
                send_diag()
            if i == middle:
                keep_own()

        @pl.when(overlaps(group))
        def _():
            relay_x(first)

        @pl.when(jnp.logical_not(overlaps(group)))
        def _():
            relay_x(middle)

        @pl.when(overlaps(group))
        def _():
            for k, source in sources:
                for t in range(col_cap):
                    for child in range(2):
                        cols_out[source, t, child] = project(
                            child, rows_out[source, 2 * t + par, child]
                        )
                    for p in range(2):
                        side_copy(k, source, t, p).start()

    @pl.when(jnp.logical_not(holder))
    def _():
        send_pair()
        keep_own()
        send_diag()

        @pl.when(z_over)
        def _():
            relay_z(first, last)

        @pl.when(jnp.logical_not(z_over))
        def _():
            relay_z(middle, len(steps))

    @pl.when(jnp.logical_and(jnp.logical_not(overlaps(group)), core == 1))
    def _():
        for t in range(col_cap):
            for p in range(2):
                for k, source in sources:
                    both = col_part(source, t, p)
                    all_of(both, col_send.at[k - 1], col_recv.at[k - 1, 2 * t + p]).wait_recv()
                    side_copy(k, source, t, p).start()

    load(front_out, front_out, 2).wait()

    @pl.when(row == diag_row)
    def _():
        all_of(sum_diag, diag_send, diag_recv.at[group]).wait_recv()
        add_diag(group)

    all_of(pair_rows, pair_send, pair_recv).wait_recv()
    all_of(pair_rows, pair_send, pair_recv).wait_send()
    all_of(cols_out.at[group, :, 1 - core], near_send, near_recv).wait_recv()
    all_of(cols_out.at[group, :, core], near_send, near_recv).wait_send()
    for k, dest in far:
        all_of(far_rows.at[k - 1], far_send.at[k - 1], relay_recv.at[k - 1, 0]).wait_send()

    swap_copy().wait_send()

    @pl.when(row != diag_row)
    def _():
        diag_copy().wait_send()

    for k, dest in far:
        @pl.when(jnp.logical_not(overlaps(dest)))
        def _():
            all_of(cols_out.at[group, :, core], col_send.at[k - 1], side_recv.at[k - 1]).wait_send()

        @pl.when(overlaps(dest))
        def _():
            all_of(extra_rows, extra_send, extra_recv.at[k - 1]).wait_send()

    @pl.when(row == diag_row)
    def _():
        for k, source in sources:
            all_of(diag_in.at[source], diag_send, diag_recv.at[source]).wait_recv()
            add_diag(source)

    end = len(steps)

    def rows_of(low, high):
        return rows_out.at[group, 0, :, pl.ds(0, sum(size for _, _, size in steps[low:high]))]

    def relayed(k, low, high, way):
        return all_of(rows_of(low, high), relay_send.at[k - 1], relay_recv.at[k - 1, way])

    @pl.when(holder)
    def _():
        for k, source in sources:
            all_of(rows_of(middle, end), both_send.at[k - 1], z_recv.at[k - 1, middle]).wait_recv()
            all_of(rows_out.at[group], both_send.at[k - 1], z_recv.at[k - 1, 0]).wait_send()

            @pl.when(overlaps(group))
            def _():
                for i in range(first, middle):
                    z_copy(k, source, 1 - par, i).wait_recv()
                relayed(k, 0, first, 0).wait_send()

            @pl.when(jnp.logical_not(overlaps(group)))
            def _():
                relayed(k, 0, middle, 0).wait_send()

    @pl.when(jnp.logical_not(holder))
    def _():
        for k, source in sources:
            for i in range(first):
                x_copy(k, source, par, i).wait_recv()

            @pl.when(z_over)
            def _():
                for i in range(last, len(steps)):
                    x_copy(k, source, par, i).wait_recv()
                relayed(k, first, last, 0).wait_send()

            @pl.when(jnp.logical_not(z_over))
            def _():
                for i in range(first, middle):
                    x_copy(k, source, par, i).wait_recv()
                relayed(k, middle, end, 0).wait_send()

            @pl.when(overlaps(group))
            def _():
                all_of(rows_of(last, end), extra_send, extra_recv.at[k - 1]).wait_recv()
                relayed(k, 0, first, 0).wait_recv()
                relayed(k, first, last, 1).wait_recv()

            @pl.when(jnp.logical_not(overlaps(group)))
            def _():
                relayed(k, 0, middle, 0).wait_recv()
                relayed(k, middle, end, 1).wait_recv()

    gives = jnp.where(overlaps(group), holder, core == 1)
    for k, source in sources:
        side = all_of(cols_out.at[source], side_send.at[k - 1], side_recv.at[k - 1])

        @pl.when(gives)
        def _():
            side.wait_send()

        @pl.when(jnp.logical_not(gives))
        def _():
            side.wait_recv()


def add_kernel(
    front_ref, rows_ref, cols_ref, out_ref, staged, out_sem
):
    rows_local, halves, block, cols_local, _ = front_ref.shape
    _, row_cap, _, _, rank = rows_ref.shape
    col_cap = cols_ref.shape[1]

    for a in range(rows_local):
        s, m = divmod(a, row_cap)
        cuts = (0, block // 2, block) if a < 4 else (0, block)
        for low, high in zip(cuts[:-1], cuts[1:]):
            size = high - low
            rows = jnp.concatenate(
                [rows_ref[s, m, 0, low:high], rows_ref[s, m, 1, low:high]], axis=1
            )
            for b in range(cols_local):
                cols = cols_ref[b // col_cap, b % col_cap].reshape(2 * rank, block)
                tile = jnp.dot(rows, cols, preferred_element_type=jnp.float32)
                spot = pl.ds(low * cols_local + b, size, stride=cols_local)
                for h in range(halves):
                    src = front_ref.at[a, h].reshape(block * cols_local, LANES)
                    dst = staged.at[a, h].reshape(block * cols_local, LANES)
                    dst[spot, :] = src[spot, :] + tile[:, h * LANES:(h + 1) * LANES]
            for h in range(halves):
                pltpu.make_async_copy(
                    staged.at[a, h, low:high], out_ref.at[a, low:high, h], out_sem
                ).start()
    pltpu.make_async_copy(staged, staged, out_sem).wait()


def shards(parent_front, generators, diagonal_blocks, coupling, block_map, valid_rows):
    row_count = lax.axis_size("row")
    col_count = lax.axis_size("col")
    groups = row_count // 2
    block, rank = generators.shape[1:]
    rows_local = parent_front.shape[0]
    cols_local = parent_front.shape[2]
    row_cap = rows_local // groups
    col_cap = cols_local // groups
    vmem = pl.BlockSpec(memory_space=pltpu.VMEM)
    hbm = pl.BlockSpec(memory_space=pltpu.HBM)
    dma = pltpu.SemaphoreType.DMA
    halves = block // LANES
    split = parent_front.reshape(rows_local, block, cols_local, halves, LANES)
    split = split.transpose(0, 1, 3, 2, 4)
    held = (rows_local, halves, block, cols_local, LANES)
    operands = [
        pltpu.with_memory_space_constraint(x, pltpu.HBM)
        for x in (generators, diagonal_blocks, coupling, block_map, valid_rows, split)
    ]
    far = groups - 1
    group_blocks = generators.shape[0]
    near = (far, row_cap * row_count - group_blocks + 1, block, rank)
    extra = (col_cap * block * sum(SIZES[LAST_AT:]) // UNITS, rank)
    rows, cols, front = pl.pallas_call(
        functools.partial(exchange_kernel, row_count, col_count, row_cap, col_cap),
        out_shape=(
            pltpu.VMEM((groups, row_cap, 2, block, rank), jnp.bfloat16),
            pltpu.VMEM((groups, col_cap, 2, rank, block), jnp.bfloat16),
            pltpu.VMEM(held, jnp.float32),
        ),
        in_specs=[hbm] * 6,
        out_specs=(vmem,) * 3,
        scratch_shapes=[
            pltpu.VMEM(generators.shape, jnp.bfloat16),
            pltpu.VMEM(near, jnp.bfloat16),
            pltpu.VMEM(diagonal_blocks.shape, jnp.bfloat16),
            pltpu.VMEM(coupling.shape, jnp.bfloat16),
            pltpu.SMEM(block_map.shape, jnp.int32),
            pltpu.SMEM(valid_rows.shape, jnp.int32),
            dma((4,)),
            pltpu.VMEM((far, col_cap, block, rank), jnp.bfloat16),
            pltpu.VMEM(extra, jnp.bfloat16),
            pltpu.VMEM((row_cap, block, rank), jnp.bfloat16),
            pltpu.VMEM((col_cap * block, block), jnp.bfloat16),
            pltpu.VMEM((col_cap * block // 2, block), jnp.bfloat16),
            pltpu.VMEM((col_cap * block // 2, block), jnp.bfloat16),
            pltpu.VMEM((groups, col_cap * block, block), jnp.bfloat16),
            dma((far,)),
            dma((far, len(SIZES))),
            dma((far,)),
            dma((far, HALF_AT + 1)),
            dma((far,)),
            dma((far, 2)),
            dma,
            dma,
            dma,
            dma,
            dma((far,)),
            dma((far, 2 * col_cap)),
            dma((far,)),
            dma((far,)),
            dma,
            dma,
            dma,
            dma((groups,)),
            dma,
            dma((far,)),
        ],
        compiler_params=pltpu.CompilerParams(
            collective_id=0, has_side_effects=True, vmem_limit_bytes=32 * 1024 * 1024
        ),
    )(*operands)
    out = pl.pallas_call(
        add_kernel,
        out_shape=jax.ShapeDtypeStruct(split.shape, jnp.float32),
        in_specs=[vmem] * 3,
        out_specs=hbm,
        scratch_shapes=[pltpu.VMEM(held, jnp.float32), dma],
        compiler_params=pltpu.CompilerParams(vmem_limit_bytes=32 * 1024 * 1024),
    )(*(pltpu.with_memory_space_constraint(x, pltpu.VMEM) for x in (front, rows, cols)))
    return out.transpose(0, 1, 3, 2, 4).reshape(parent_front.shape)


def solution(mesh):
    in_specs = (
        P(None, "row", None, "col"),
        P("row", None, None),
        P("row", None, None),
        P(),
        P(),
        P(),
    )
    out_specs = P(None, "row", None, "col")
    return jax.shard_map(shards, mesh=mesh, in_specs=in_specs, out_specs=out_specs, check_vma=False)
```
